32 devices in a mesh: dp: 8 (over y, x, core), expert: 4 (over z).
Axes of the slice: x: 2, y: 2, z: 4, core: 2. Of those that a mesh axis runs over, the one named last changes fastest.
Arguments:
- tokens: bfloat16 [512, 4096], P('expert', 'dp'), may hold values from -6 to 6
- in_signs: int32 [512, 128], P('expert', 'dp'), may hold values from -2147483648 to 2147483646
- out_signs: int32 [512, 224], P('expert'), may hold values from -2147483648 to 2147483646
- expert_ids: int32 [512, 2], P('expert'), may hold values from 0 to 3, all different within a row; in each aligned block of 128 rows (0 to 127, 128 to 255, ...) at most 80 rows name the same one
- route_weight: float32 [512, 2], P('expert'), may hold values from 0.2 to 1
- cotangent: bfloat16 [512, 7168], P('expert', 'dp'), may hold values from -6 to 6
- mean_weight: bfloat16 [4, 4096, 7168], P('expert', 'dp'), may hold values from -0.09375 to 0.09375
- rho_weight: bfloat16 [4, 4096, 7168], P('expert', 'dp'), may hold values from -6 to -3
- noise_weight: bfloat16 [4, 4096, 7168], P('expert', 'dp'), may hold values from -4 to 4
Outputs:
- hidden_out: bfloat16 [512, 7168], P('expert', 'dp')
- grad_tokens: bfloat16 [512, 4096], P('expert', 'dp')
- grad_mean: bfloat16 [4, 4096, 7168], P('expert', 'dp')
- grad_rho: bfloat16 [4, 4096, 7168], P('expert', 'dp')
The draws below stay inside these ranges and needn't reach their ends.
Inputs may be any that keep to these rules, and one draw needn't show every extreme that they name: `expert_ids`: each token names 2 different experts. In each aligned block of 128 tokens no expert is named by more than 80 tokens, and in some blocks one expert is named by exactly 80. `in_signs`: bit b of word w, counted from the lowest, is set where the sign of feature 32 * w + b is -1 and clear where it is +1. `out_signs`: bit b of word w, counted from the lowest, is set where the sign of hidden unit 32 * w + b is -1 and clear where it is +1.
All inputs are finite; a program needn't handle non-finite values.
Results may differ from the reference program's by a relative error of at most 0.0071.
Values may be sent and summed in bfloat16 or wider, within the bound.
A program may use at most 128 MiB of HBM per device.

```python
import math
import jax
import jax.numpy as jnp
import numpy as np
from jax import lax

D = 4096
FF = 7168
TOPK = 2
TOK_DEV = 128
EXPERTS = 4
CAP = 80
TOKENS = 512
N_EXPERT = 4


def with_ends(array, stream_key, low, top_value):
    shape = array.shape
    index_at = [jax.random.randint(jax.random.fold_in(stream_key, axis), (), 0, shape[axis]) for axis in range(len(shape))]
    array = array.at[tuple(index_at)].set(low)
    longest = shape.index(max(shape))
    index_at[longest] = (index_at[longest] + 1) % shape[longest]
    return array.at[tuple(index_at)].set(top_value)


def block_scale(rng, extent, pieces, least, high):
    def one(axis_at, blocks):
        steps = jax.random.uniform(jax.random.fold_in(jax.random.fold_in(rng, 6), axis_at), (blocks,), jnp.float32, least / len(pieces), high / len(pieces))
        return jnp.repeat(jnp.exp(steps), extent[axis_at] // blocks).reshape((-1,) + (1,) * (len(extent) - axis_at - 1))

    loudness = one(*pieces[0])
    for cut in pieces[1:]:
        loudness = loudness * one(*cut)
    return loudness


def shared_out(key, own, number, rows, number_of, top, limit, skew):
    ranking = jax.random.permutation(key, number_of)
    heavy_load, common = shares(number_of, rows * top, limit, skew, True), shares(number_of, rows * top, limit, skew, False)
    places = jnp.arange(number_of)

    def named(sizes, turn):
        used = int((sizes > 0).sum())
        fixed = max(1, used // 4)
        moved = fixed + (places - fixed + turn * (used - fixed)) % max(1, number_of - fixed)
        return jnp.zeros((number_of,), jnp.int32).at[ranking[jnp.where(places < fixed, places, moved)]].set(jnp.asarray(sizes, jnp.int32))

    sizes = jnp.where(number % 4 == 0, named(heavy_load, number // 4), named(common, number - number // 4 - 1))
    mixed = jax.random.permutation(jax.random.fold_in(own, 3), number_of)
    giver, sink = mixed[0:number_of // 2 * 2:2], mixed[1:number_of // 2 * 2:2]
    slack = jnp.minimum(sizes[giver] - 1, limit - sizes[sink]) // 2
    slack = jnp.where((giver == ranking[0]) | (sink == ranking[0]) | (sizes[sink] == 0), 0, jnp.maximum(slack, 0))
    moved = jax.random.randint(jax.random.fold_in(own, 4), (number_of // 2,), 0, 1 << 20) % (slack + 1)
    sizes = sizes.at[giver].add(-moved).at[sink].add(moved)
    members = jnp.searchsorted(jnp.cumsum(sizes), jnp.arange(rows * top), side="right").astype(jnp.int32)
    listing = members.reshape(top, rows).T
    listing = listing[jax.random.permutation(jax.random.fold_in(own, 1), rows)]
    turn = jax.random.randint(jax.random.fold_in(own, 2), (rows, 1), 0, top)
    return jnp.take_along_axis(listing, (jnp.arange(top)[None, :] + turn) % top, axis=1)


def shares(count, total, limit, skew, full):
    weights = [(1 << 20) // math.isqrt(grade ** skew) + 1 for grade in range(1, count + 1)]
    largest = limit if full else min(limit, max(-(-total // count), total * weights[0] // sum(weights)))
    least = 1 if total - largest >= count - 1 else 0
    holding, surplus = [largest] + [least] * (count - 1), total - largest - least * (count - 1)
    while surplus > 0:
        free = [i for i in range(1, count) if holding[i] < largest] or [i for i in range(1, count) if holding[i] < limit]
        whole, remaining = sum([weights[i] for i in free]), surplus
        for i in free:
            more = min(limit - holding[i], max(1, remaining * weights[i] // whole), surplus)
            holding[i] = holding[i] + more
            surplus = surplus - more
    return np.array(holding)


def bell_draw(key, dims, deviation, most, cuts=(), kind=jnp.bfloat16):
    entries = jax.random.normal(key, dims, jnp.float32) * deviation
    if len(cuts) > 0:
        entries = block_scale(key, dims, cuts, -0.22, 0.18) * entries
    return jnp.clip(entries, min=-most, max=most).astype(kind)


def setup_inputs(seed: int = 0) -> dict:
    key_list = jax.random.split(jax.random.key(seed), 10)
    tokens = bell_draw(key_list[0], (TOKENS, D), 1.0, 6.0, ((0, 4), (1, 8)))
    in_signs = with_ends(jax.random.randint(key_list[1], (TOKENS, D // 32), -2147483648, 2147483647), jax.random.fold_in(key_list[1], 1), -2147483648, 2147483646).astype(jnp.int32)
    out_signs = with_ends(jax.random.randint(key_list[2], (TOKENS, FF // 32), -2147483648, 2147483647), jax.random.fold_in(key_list[2], 1), -2147483648, 2147483646).astype(jnp.int32)
    expert_ids_keys = jax.random.split(jax.random.fold_in(key_list[3], 1), TOKENS // TOK_DEV)
    expert_ids_turns = jax.random.permutation(jax.random.fold_in(key_list[3], 3), TOKENS // TOK_DEV)
    expert_ids = jax.vmap(lambda own, number: shared_out(jax.random.fold_in(key_list[3], 2), own, number, TOK_DEV, EXPERTS, TOPK, CAP, 2))(expert_ids_keys, expert_ids_turns).reshape((TOKENS, TOPK))
    route_weight = jnp.clip(0.2 + 0.8 * jax.random.uniform(key_list[4], (TOKENS, TOPK), jnp.float32) ** block_scale(key_list[4], (TOKENS, TOPK), ((0, 4),), -0.2, 0.2), 0.2, 1.0)
    cotangent = bell_draw(key_list[5], (TOKENS, FF), 1.0, 6.0, ((0, 4), (1, 8)))
    mean_weight = bell_draw(key_list[6], (EXPERTS, D, FF), D ** -0.5, 0.09375, ((0, 4), (1, 8)))
    rho_weight = jnp.clip(-6.0 + 3.0 * jax.random.uniform(key_list[7], (EXPERTS, D, FF), jnp.float32) ** block_scale(key_list[7], (EXPERTS, D, FF), ((0, 4), (1, 8)), -0.2, 0.2), -6.0, -3.0).astype(jnp.bfloat16)
    noise_weight = bell_draw(key_list[8], (EXPERTS, D, FF), 1.0, 4.0, ((0, 4), (1, 8)))
    return dict(tokens=tokens, in_signs=in_signs, out_signs=out_signs, expert_ids=expert_ids, route_weight=route_weight, cotangent=cotangent, mean_weight=mean_weight, rho_weight=rho_weight, noise_weight=noise_weight)


def unpack_rows(words):
    shifts = jnp.arange(32, dtype=jnp.int32)
    bits = jnp.bitwise_and(jnp.right_shift(words[..., None], shifts), 1)
    signs = (1 - 2 * bits).astype(jnp.float32)
    return signs.reshape(words.shape[:-1] + (words.shape[-1] * 32,))


def block_slots(block_ids):
    onehot = (block_ids[:, :, None] == jnp.arange(EXPERTS, dtype=jnp.int32)).astype(jnp.int32)
    flat = onehot.reshape(-1, EXPERTS)
    before = (jnp.cumsum(flat, axis=0) - flat).astype(jnp.int32)
    return jnp.sum(before * flat, axis=1).astype(jnp.int32).reshape(block_ids.shape)


def reference(tokens, in_signs, out_signs, expert_ids, route_weight, cotangent, mean_weight, rho_weight, noise_weight):
    blocks = expert_ids.reshape(N_EXPERT, TOK_DEV, TOPK)
    ranks = jax.vmap(block_slots)(blocks)
    source = jnp.arange(N_EXPERT, dtype=jnp.int32)[:, None, None]
    per_expert = N_EXPERT * CAP
    position = (blocks * per_expert + source * CAP + ranks).astype(jnp.int32).reshape(TOKENS, TOPK)
    total = EXPERTS * per_expert
    token_index = jnp.broadcast_to(jnp.arange(TOKENS, dtype=jnp.int32)[:, None], (TOKENS, TOPK))
    flat_pos = position.reshape(-1)
    slot_token = jnp.zeros((total,), jnp.int32).at[flat_pos].set(token_index.reshape(-1))
    slot_fill = jnp.zeros((total,), jnp.float32).at[flat_pos].set(1.0)
    slot_weight = jnp.zeros((total,), jnp.float32).at[flat_pos].set(route_weight.reshape(-1))
    input_full = unpack_rows(in_signs)
    output_full = unpack_rows(out_signs)

    def one_expert(operands):
        mean_e, rho_e, noise_e, tok_e, fill_e, weight_e = operands
        rows = jnp.take(tokens, tok_e, axis=0) * fill_e[:, None].astype(jnp.bfloat16)
        input_rows = jnp.take(input_full, tok_e, axis=0)
        output_rows = jnp.take(output_full, tok_e, axis=0)
        signed = rows * input_rows.astype(jnp.bfloat16)
        rho_float = rho_e.astype(jnp.float32)
        noise_float = noise_e.astype(jnp.float32)
        delta = (jax.nn.softplus(rho_float) * noise_float).astype(jnp.bfloat16)
        mean_part = jnp.dot(rows, mean_e, preferred_element_type=jnp.float32)
        pert_part = jnp.dot(signed, delta, preferred_element_type=jnp.float32)
        preact = mean_part + output_rows * pert_part
        gate = jax.nn.sigmoid(preact)
        hidden = (preact * gate).astype(jnp.bfloat16)
        upstream = (jnp.take(cotangent, tok_e, axis=0).astype(jnp.float32) * weight_e[:, None]).astype(jnp.bfloat16)
        slope = gate * (1.0 + preact * (1.0 - gate))
        grad_preact = (upstream.astype(jnp.float32) * slope).astype(jnp.bfloat16)
        grad_signed_pre = grad_preact * output_rows.astype(jnp.bfloat16)
        grad_mean_e = jnp.dot(rows.T, grad_preact, preferred_element_type=jnp.float32).astype(jnp.bfloat16)
        grad_delta = jnp.dot(signed.T, grad_signed_pre, preferred_element_type=jnp.float32)
        grad_rho_e = (grad_delta * noise_float * jax.nn.sigmoid(rho_float)).astype(jnp.bfloat16)
        back = jnp.dot(grad_preact, mean_e.T, preferred_element_type=jnp.float32)
        back = back + input_rows * jnp.dot(grad_signed_pre, delta.T, preferred_element_type=jnp.float32)
        return hidden, back.astype(jnp.bfloat16), grad_mean_e, grad_rho_e

    operands = (mean_weight, rho_weight, noise_weight, slot_token.reshape(EXPERTS, per_expert),
                slot_fill.reshape(EXPERTS, per_expert), slot_weight.reshape(EXPERTS, per_expert))
    hidden_slots, back_slots, grad_mean, grad_rho = lax.map(one_expert, operands)
    picked = jnp.take(hidden_slots.reshape(total, FF), position, axis=0).astype(jnp.float32)
    hidden_out = jnp.sum(picked * route_weight[:, :, None], axis=1).astype(jnp.bfloat16)
    returned = jnp.take(back_slots.reshape(total, D), position, axis=0).astype(jnp.float32)
    grad_tokens = jnp.sum(returned, axis=1).astype(jnp.bfloat16)
    return hidden_out, grad_tokens, grad_mean, grad_rho
```

```python
import functools

import jax
import jax.numpy as jnp
from jax import lax
from jax.experimental import pallas as pl
from jax.experimental.pallas import tpu as pltpu
from jax.sharding import PartitionSpec as P

def unpack_rows(words):
    shifts = jnp.arange(32, dtype=jnp.int32)
    bits = jnp.bitwise_and(jnp.right_shift(words[..., None], shifts), 1)
    signs = (1 - 2 * bits).astype(jnp.float32)
    return signs.reshape(words.shape[:-1] + (words.shape[-1] * 32,))


def unpack_cols(words):
    shifts = jnp.arange(32, dtype=jnp.int32)
    bits = jnp.bitwise_and(jnp.right_shift(words.T[:, None, :], shifts[None, :, None]), 1)
    signs = (1 - 2 * bits).astype(jnp.float32)
    return signs.reshape(words.shape[1] * 32, words.shape[0])


def block_slots(block_ids, experts, capacity):
    onehot = (block_ids[:, :, None] == jnp.arange(experts, dtype=jnp.int32)).astype(jnp.int32)
    flat = onehot.reshape(-1, experts)
    before = jnp.cumsum(flat, axis=0) - flat
    ranks = jnp.sum(before * flat, axis=1).reshape(block_ids.shape)
    return block_ids * capacity + ranks


def on_device_general(
    tokens,
    in_signs,
    out_signs,
    expert_ids,
    route_weight,
    cotangent,
    mean_weight,
    rho_weight,
    noise_weight,
):
    experts = lax.axis_size("expert") * mean_weight.shape[0]
    token_count = tokens.shape[0]
    topk = expert_ids.shape[1]
    capacity = 5 * token_count * topk // (4 * experts)
    slots = experts * capacity
    width_local = tokens.shape[1]
    sign_words = in_signs.shape[1]
    hidden_local = cotangent.shape[1]
    slot_of = block_slots(expert_ids, experts, capacity)
    match = (slot_of[:, :, None] == jnp.arange(slots, dtype=jnp.int32)).astype(jnp.int32)
    token_rank = jnp.arange(token_count, dtype=jnp.int32)[:, None, None]
    slot_token = jnp.sum(match * token_rank, axis=(0, 1))
    slot_fill = jnp.sum(match, axis=(0, 1))
    slot_weight = jnp.sum(match.astype(jnp.float32) * route_weight[:, :, None], axis=(0, 1))
    words = jnp.concatenate([in_signs, out_signs], axis=1)
    fill_rows = slot_fill.astype(jnp.bfloat16)[:, None]
    send_rows = (jnp.take(tokens, slot_token, axis=0) * fill_rows).reshape(
        experts, capacity, width_local
    )
    send_words = jnp.take(words, slot_token, axis=0).reshape(experts, capacity, words.shape[1])
    recv_rows, recv_words = (
        lax.all_to_all(send_rows, "expert", split_axis=0, concat_axis=0, tiled=True),
        lax.all_to_all(send_words, "expert", split_axis=0, concat_axis=0, tiled=True),
    )
    rows = recv_rows.reshape(slots, width_local)
    recv_words = recv_words.reshape(slots, words.shape[1])
    input_signs = unpack_rows(recv_words[:, :sign_words])
    input_cols = unpack_cols(recv_words[:, :sign_words])
    signed = rows * input_signs.astype(jnp.bfloat16)
    mean_local = mean_weight[0]
    rho_float = rho_weight[0].astype(jnp.float32)
    noise_float = noise_weight[0].astype(jnp.float32)
    delta = (jax.nn.softplus(rho_float) * noise_float).astype(jnp.bfloat16)
    contract = (((0,), (1,)), ((), ()))
    output_cols = unpack_cols(recv_words[:, sign_words:])
    mean_cols = mean_local
    delta_cols = delta
    mean_part = lax.dot_general(mean_cols, rows, contract, preferred_element_type=jnp.float32)
    pert_part = lax.dot_general(delta_cols, signed, contract, preferred_element_type=jnp.float32)
    mean_part, pert_part = (mean_part, pert_part)
    preact = lax.psum_scatter(
        mean_part + output_cols * pert_part, "dp", scatter_dimension=0, tiled=True
    )
    gate = jax.nn.sigmoid(preact)
    hidden_slots = (preact * gate).astype(jnp.bfloat16)
    slope = gate * (1.0 + preact * (1.0 - gate))
    returned = lax.all_to_all(
        hidden_slots.reshape(hidden_local, experts, capacity),
        "expert",
        split_axis=1,
        concat_axis=1,
        tiled=True,
    )
    returned = returned.reshape(hidden_local, slots)
    picked = jnp.take(returned, slot_of, axis=1).astype(jnp.float32)
    hidden_out = jnp.sum(picked * route_weight[None], axis=2).T.astype(jnp.bfloat16)
    upstream = jnp.take(cotangent.T, slot_token, axis=1).astype(jnp.float32) * slot_weight[None, :]
    upstream = upstream.astype(jnp.bfloat16).reshape(hidden_local, experts, capacity)
    arrived = lax.all_to_all(upstream, "expert", split_axis=1, concat_axis=1, tiled=True).reshape(
        hidden_local, slots
    )
    grad_preact = (arrived.astype(jnp.float32) * slope).astype(jnp.bfloat16)
    piece = lax.all_gather(grad_preact, "dp", axis=0, tiled=True)
    piece_signed = piece * output_cols.astype(jnp.bfloat16)
    mean_cols = mean_local
    delta_cols = delta
    grad_rows = jnp.dot(mean_cols, piece, preferred_element_type=jnp.float32)
    grad_signed = jnp.dot(delta_cols, piece_signed, preferred_element_type=jnp.float32)
    mean_block = lax.dot_general(rows, piece, contract, preferred_element_type=jnp.float32)
    delta_block = lax.dot_general(
        signed, piece_signed, contract, preferred_element_type=jnp.float32
    )
    grad_mean_acc = mean_block
    grad_delta_acc = delta_block
    result = (grad_rows, grad_signed, grad_mean_acc, grad_delta_acc)
    grad_rows, grad_signed, grad_mean_acc, grad_delta_acc = result
    slot_grad = (grad_rows + input_cols * grad_signed).astype(jnp.bfloat16)
    back = lax.all_to_all(
        slot_grad.reshape(width_local, experts, capacity),
        "expert",
        split_axis=1,
        concat_axis=1,
        tiled=True,
    )
    back = back.reshape(width_local, slots)
    grad_tokens = jnp.sum(jnp.take(back, slot_of, axis=1).astype(jnp.float32), axis=2).T.astype(
        jnp.bfloat16
    )
    grad_mean = grad_mean_acc.astype(jnp.bfloat16)[None]
    grad_rho = (grad_delta_acc * noise_float * jax.nn.sigmoid(rho_float)).astype(jnp.bfloat16)[None]
    return (hidden_out, grad_tokens, grad_mean, grad_rho)


LANES = 128
VMEM_LIMIT = 60 * 1024 * 1024
RANKS = 4
COPIES = 80
NT = (((1,), (1,)), ((), ()))
TN = (((0,), (0,)), ((), ()))
ORDER = (7, 6, 3, 2, 5, 4, 1, 0)


def dot(a, b, dims=None):
    if dims is None:
        return jnp.dot(a, b, preferred_element_type=jnp.float32)
    return lax.dot_general(a, b, dims, preferred_element_type=jnp.float32)


def total(*terms):
    out = terms[0].astype(jnp.float32)
    for term in terms[1:]:
        out = out + term.astype(jnp.float32)
    return out


def signs_of(words, first, tiles):
    rows = words.shape[0]
    lane = lax.broadcasted_iota(jnp.int32, (rows, LANES), 1)
    shift = lane % 32
    out = []
    for tile in range(tiles):
        at = first + 4 * tile + lane // 32
        picked = jnp.take_along_axis(words, at, axis=1, mode="promise_in_bounds")
        bits = jnp.bitwise_and(jnp.right_shift(picked, shift), 1)
        out.append((1 - 2 * bits).astype(jnp.float32).astype(jnp.bfloat16))
    return jnp.concatenate(out, axis=1) if tiles > 1 else out[0]


def step_kernel(
    ids_ref, weight_ref, tok_ref, cot_ref, inw_ref, outw_ref, mean_hbm, rho_hbm, noise_hbm,
    hid_ref, fill_ref, g_ref, at_ref, bt_ref, dy_hbm, dyr_hbm, q_hbm,
    mean_v, delta_v, q_v, part, r_v, dy_v, rd, cs, land, xs, bs, ss, send_x,
    words_s, words_v, raw, up_s, up_v, h_s, h_v, one_v, plain, signed,
    send_sem, recv_sem, local_sem,
):
    bf16, f32 = jnp.bfloat16, jnp.float32
    me = lax.axis_index("dp")
    mine = lax.axis_index("expert")
    tokens = tok_ref.shape[0]
    width = tok_ref.shape[1]
    block = cot_ref.shape[1]
    cap = up_v.shape[1]
    pair = 2 * cap
    slots = RANKS * cap
    in_words = inw_ref.shape[0]
    half_words = outw_ref.shape[0] // 2
    piece_words = block // 32
    y, x, c = me // 4, (me // 2) % 2, me % 2
    place = lambda dy, dx, dc: ((y + dy) % 2) * 4 + ((x + dx) % 2) * 2 + (c + dc) % 2
    owner = [place(l // 4, (l // 2) % 2, l % 2) for l in range(8)]
    at_x, at_y, at_c = (place(0, 1, 0), mine), (place(1, 0, 0), mine), (place(0, 0, 1), mine)
    zs = [mine, mine + 1 - 2 * (mine % 2), (mine + 2) % 4, 3 - mine]
    at_z = [(me, z) for z in zs]
    count = [0, 0]
    started, copied = [], []

    def send(src, dst, to):
        n = count[0]
        count[0] += 1
        copy = pltpu.make_async_remote_copy(
            src_ref=src,
            dst_ref=dst,
            send_sem=send_sem.at[n],
            recv_sem=recv_sem.at[n],
            device_id=to,
            device_id_type=pl.DeviceIdType.MESH,
        )
        copy.start()
        started.append(copy)
        return copy

    def local(src, dst, keep=True):
        n = count[1]
        count[1] += 1
        copy = pltpu.make_async_copy(src, dst, local_sem.at[n])
        copy.start()
        if keep:
            copied.append(copy)
        return copy

    cols = [pl.ds(pl.multiple_of(owner[l] * block, LANES), block) for l in range(8)]
    got = {}
    for l in ORDER:
        got[l] = (
            local(rho_hbm.at[:, cols[l]], delta_v.at[l], False),
            local(noise_hbm.at[:, cols[l]], q_v.at[l], False),
            local(mean_hbm.at[:, cols[l]], mean_v.at[l], False),
        )

    barrier = pltpu.get_barrier_semaphore()
    peers = [at_x, at_y, at_c] + at_z[1:]
    for peer in peers:
        pl.semaphore_signal(barrier, inc=1, device_id=peer, device_id_type=pl.DeviceIdType.MESH)

    ids = ids_ref[...]
    weight = weight_ref[...]
    id0, id1 = ids[0:1, :], ids[1:2, :]
    w0, w1 = weight[0:1, :], weight[1:2, :]
    sub16 = lax.broadcasted_iota(jnp.int32, (16, tokens), 0)
    named = jnp.zeros((16, tokens), f32)
    for j in range(RANKS):
        hit = jnp.where(id0 == zs[j], 1.0, 0.0) + jnp.where(id1 == zs[j], 1.0, 0.0)
        named = jnp.where(sub16 == j, jnp.broadcast_to(hit, (16, tokens)), named)
    row_at = lax.broadcasted_iota(jnp.int32, (tokens, tokens), 0)
    col_at = lax.broadcasted_iota(jnp.int32, (tokens, tokens), 1)
    earlier = jnp.where(row_at < col_at, 1.0, 0.0).astype(bf16)
    ranks = dot(named.astype(bf16), earlier)
    slot_at = lax.broadcasted_iota(jnp.int32, (cap, tokens), 0).astype(f32)
    slot_weight = []
    for j in range(RANKS):
        rows = pl.ds(j * cap, cap)
        here = jnp.where(slot_at == ranks[j : j + 1, :], 1.0, 0.0)
        one = here * jnp.where(id0 == zs[j], 1.0, 0.0)
        two = here * jnp.where(id1 == zs[j], 1.0, 0.0)
        one_v[0, rows] = one.astype(bf16)
        one_v[1, rows] = two.astype(bf16)
        fill_ref[rows] = (one + two).astype(bf16)
        slot_weight.append(jnp.sum(one * w0 + two * w1, axis=1, keepdims=True))
    fill = fill_ref[...]
    taken = dot(fill, tok_ref[...]).astype(bf16)
    xs[pl.ds(0, cap)] = taken[:cap]
    send_x[...] = taken
    words_s[pl.ds(0, half_words)] = outw_ref[pl.ds(pl.multiple_of(c * half_words, 8), half_words)]
    words_s[pl.ds(half_words, in_words)] = inw_ref[...]
    words = words_s[...]
    gathered = None
    for k in range(4):
        plane = jnp.bitwise_and(jnp.right_shift(words, 8 * k), 255).astype(f32).astype(bf16)
        got_plane = jnp.left_shift(dot(fill, plane, NT).astype(jnp.int32), 8 * k)
        gathered = got_plane if k == 0 else jnp.bitwise_or(gathered, got_plane)
    raw[...] = gathered
    words_v[c, pl.ds(0, cap)] = gathered[:cap]

    pl.semaphore_wait(barrier, len(peers))
    block_rows = [pl.ds(j * cap, cap) for j in range(RANKS)]
    pair_rows = [pl.ds(0, pair), pl.ds(pair, pair)]
    x_in, w_in, w_swap, up_in = {}, {}, {}, {}

    def send_rows(j):
        x_in[j] = send(send_x.at[block_rows[j]], xs.at[block_rows[j]], at_z[j])

    def send_words(j):
        w_in[j] = send(raw.at[block_rows[j]], words_v.at[c, block_rows[j]], at_z[j])

    def swap_words(j):
        here = words_v.at[c, block_rows[j]]
        w_swap[j] = send(here, here, at_c)

    send_rows(1)
    send_words(1)
    send_rows(2)
    send_rows(3)
    send_words(2)
    send_words(3)
    swap_words(0)

    def make_delta(l):
        got[l][0].wait()
        got[l][1].wait()

        @pl.loop(0, width // 32)
        def _(i):
            rows = pl.ds(pl.multiple_of(i * 32, 32), 32)
            rho = delta_v[l, rows].astype(f32)
            noise = q_v[l, rows].astype(f32)
            soft = jnp.log(1.0 + jnp.exp(rho))
            delta_v[l, rows] = (soft * noise).astype(bf16)
            q_v[l, rows] = (jnp.exp(rho - soft) * noise).astype(bf16)

    for l in ORDER[:3]:
        make_delta(l)
    up = dot(fill, cot_ref[...])
    for j in range(RANKS):
        mixed = (up[j * cap : (j + 1) * cap] * slot_weight[j]).astype(bf16)
        if j == 0:
            up_v[0] = mixed
        else:
            up_s[j] = mixed
    for j in range(1, RANKS):
        up_in[j] = send(up_s.at[j], up_v.at[j], at_z[j])
    for l in ORDER[3:5]:
        make_delta(l)
    made = set(ORDER[:5])

    def arrive(p):
        blocks = (1,) if p == 0 else (2, 3)
        for j in blocks:
            x_in[j].wait_recv()
            w_in[j].wait_recv()
            swap_words(j)
        rows = pair_rows[p]
        signs = signs_of(words_v[c, rows], half_words, width // LANES)
        ss[rows] = signs
        bs[rows] = xs[rows] * signs
        for j in (2 * p, 2 * p + 1):
            w_swap[j].wait_recv()

    def forward(p, l):
        rows = pair_rows[p]
        if l not in made:
            make_delta(l)
            made.add(l)
        if p == 0:
            got[l][2].wait()
        one = dot(xs[rows], mean_v[l])
        two = dot(bs[rows], delta_v[l])
        signs = signs_of(
            words_v[owner[l] // 4, rows], (owner[l] % 4) * piece_words, block // LANES
        )
        r_v[l, rows] = signs
        part[l, rows] = (one + signs.astype(f32) * two).astype(bf16)

    core, sent = {}, {}

    def to_core(p, k):
        rows = pair_rows[p]
        core[p, k] = send(part.at[2 * k + 1, rows], rd.at[k, rows], at_c)

    def hop(p, k, which, name, to, extra=None):
        rows = block_rows[2 * p + which]
        terms = [part[2 * k, rows], rd[k, rows]]
        if extra is not None:
            terms.append(land[p, extra])
        cs[k, rows] = total(*terms).astype(bf16)
        sent[p, name] = send(cs.at[k, rows], land.at[p, name], to)

    D_X, D_Y, N_X, N_Y, L_Y, L_X = range(6)

    def reduce_first(p, middle):
        forward(p, 7)
        to_core(p, 3)
        forward(p, 6)
        core[p, 3].wait_recv()
        hop(p, 3, 0, D_X, at_x)
        hop(p, 3, 1, D_Y, at_y)
        forward(p, 3)
        to_core(p, 1)
        forward(p, 2)
        core[p, 1].wait_recv()
        hop(p, 1, 0, N_X, at_x)
        forward(p, 5)
        to_core(p, 2)
        forward(p, 4)
        core[p, 2].wait_recv()
        hop(p, 2, 1, N_Y, at_y)
        middle()
        forward(p, 1)
        to_core(p, 0)
        forward(p, 0)

    def reduce_last(p):
        sent[p, D_X].wait_recv()
        hop(p, 2, 0, L_Y, at_y, D_X)
        sent[p, D_Y].wait_recv()
        hop(p, 1, 1, L_X, at_x, D_Y)
        core[p, 0].wait_recv()

    spread, h_in = {}, {}

    def pass_on(p, which, l, to_l, to, name):
        rows = block_rows[2 * p + which]
        spread[p, name] = send(dy_v.at[l, rows], dy_v.at[to_l, rows], to)

    def activate(p, which):
        j = 2 * p + which
        rows = block_rows[j]
        if j > 0:
            up_in[j].wait_recv()
        near, last = (N_X, L_Y) if which == 0 else (N_Y, L_X)
        sent[p, near].wait_recv()
        sent[p, last].wait_recv()
        preact = total(part[0, rows], rd[0, rows], land[p, near], land[p, last])
        gate = 1.0 / (1.0 + jnp.exp(-preact))
        hidden = (preact * gate).astype(bf16)
        slope = gate * (1.0 + preact * (1.0 - gate))
        dy_v[0, rows] = (up_v[j].astype(f32) * slope).astype(bf16)
        if j == 0:
            h_v[0] = hidden
        else:
            h_s[j] = hidden

    def gather_first(p):
        activate(p, 0)
        pass_on(p, 0, 0, 4, at_y, "y1")
        pass_on(p, 0, 0, 2, at_x, "x2")
        pass_on(p, 0, 0, 1, at_c, "c0")
        activate(p, 1)
        pass_on(p, 1, 0, 2, at_x, "x1")
        pass_on(p, 1, 0, 4, at_y, "y2")
        pass_on(p, 1, 0, 1, at_c, "c1")
        for j in (2 * p, 2 * p + 1):
            if j > 0:
                h_in[j] = send(h_s.at[j], h_v.at[j], at_z[j])

    def gather_relay(p):
        spread[p, "y1"].wait_recv()
        pass_on(p, 0, 4, 6, at_x, "x3")
        pass_on(p, 0, 4, 5, at_c, "c2")
        spread[p, "x1"].wait_recv()
        pass_on(p, 1, 2, 6, at_y, "y3")
        pass_on(p, 1, 2, 3, at_c, "c3")

    def gather_near(p):
        spread[p, "x2"].wait_recv()
        pass_on(p, 0, 2, 3, at_c, "c4")
        spread[p, "y2"].wait_recv()
        pass_on(p, 1, 4, 5, at_c, "c5")

    def gather_last(p):
        spread[p, "x3"].wait_recv()
        pass_on(p, 0, 6, 7, at_c, "c6")
        spread[p, "y3"].wait_recv()
        pass_on(p, 1, 6, 7, at_c, "c7")

    first_back = {0: True, 1: True}

    def back(p, l, waits=()):
        for name in waits:
            spread[p, name].wait_recv()
        rows = pair_rows[p]
        dy = dy_v[l, rows]
        dyr = dy * r_v[l, rows]
        r_v[l, rows] = dyr
        one = dot(dy, mean_v[l], NT)
        two = dot(dyr, delta_v[l], NT)
        if first_back[p]:
            plain[rows] = one
            signed[rows] = two
            first_back[p] = False
        else:
            plain[rows] += one
            signed[rows] += two
        if p == 1:
            local(dy_v.at[l], dy_hbm.at[:, cols[l]])
            local(r_v.at[l], dyr_hbm.at[:, cols[l]])

    arrive(0)
    reduce_first(0, lambda: None)
    reduce_last(0)
    for l in range(8):
        local(q_v.at[l], q_hbm.at[:, cols[l]])
    arrive(1)
    reduce_first(1, lambda: gather_first(0))
    reduce_last(1)
    at_ref[...] = xs[...].T
    bt_ref[...] = bs[...].T
    back(0, 0)
    back(0, 1, ("c0", "c1"))
    gather_relay(0)
    gather_first(1)
    gather_near(0)
    back(0, 2)
    back(0, 4)
    back(0, 3, ("c3", "c4"))
    back(0, 5, ("c2", "c5"))
    back(1, 0)
    back(1, 1, ("c0", "c1"))
    gather_last(0)
    back(0, 6)
    back(0, 7, ("c6", "c7"))
    gather_relay(1)
    gather_near(1)
    back(1, 2)
    back(1, 4)
    back(1, 3, ("c3", "c4"))
    back(1, 5, ("c2", "c5"))
    for j in range(1, RANKS):
        h_in[j].wait_recv()
    out = None
    for k, w in enumerate((w0, w1)):
        column = jnp.sum(jnp.where(row_at == col_at, w, 0.0), axis=1, keepdims=True)
        picked = None
        for j in range(RANKS):
            one = dot(one_v[k, block_rows[j]], h_v[j], TN)
            picked = one if picked is None else picked + one
        picked = picked * column
        out = picked if out is None else out + picked
    hid_ref[...] = out.astype(bf16)
    gather_last(1)
    back(1, 6)
    back(1, 7, ("c6", "c7"))
    g_ref[...] = (plain[...] + ss[...].astype(f32) * signed[...]).astype(bf16)
    for copy in started:
        copy.wait_send()
    for copy in copied:
        copy.wait()


def run_step(ids, weight, tokens, cotangent, in_words, out_words, mean, rho, noise, cap):
    bf16, f32 = jnp.bfloat16, jnp.float32
    width, hidden = mean.shape
    count = tokens.shape[0]
    block = cotangent.shape[1]
    slots = RANKS * cap
    vmem = pl.BlockSpec(memory_space=pltpu.VMEM)
    hbm = pl.BlockSpec(memory_space=pltpu.MemorySpace.HBM)
    shape = jax.ShapeDtypeStruct
    weights = pltpu.VMEM((8, width, block), bf16)
    piece = pltpu.VMEM((8, slots, block), bf16)
    four = pltpu.VMEM((4, slots, block), bf16)
    small = pltpu.VMEM((slots, width), bf16)
    per = pltpu.VMEM((RANKS, cap, block), bf16)
    macs = slots * width * hidden
    return pl.pallas_call(
        step_kernel,
        in_specs=[vmem] * 6 + [hbm] * 3,
        out_specs=[vmem] * 5 + [hbm] * 3,
        out_shape=[
            shape((count, block), bf16),
            shape((slots, count), bf16),
            shape((slots, width), bf16),
            shape((width, slots), bf16),
            shape((width, slots), bf16),
            shape((slots, hidden), bf16),
            shape((slots, hidden), bf16),
            shape((width, hidden), bf16),
        ],
        scratch_shapes=[
            weights, weights, weights, piece, piece, piece, four, four,
            pltpu.VMEM((2, 6, cap, block), bf16),
            small, small, small, small,
            pltpu.VMEM((LANES, count), jnp.int32),
            pltpu.VMEM((2, slots, LANES), jnp.int32),
            pltpu.VMEM((slots, LANES), jnp.int32),
            per, per, per, per,
            pltpu.VMEM((2, slots, count), bf16),
            pltpu.VMEM((slots, width), f32),
            pltpu.VMEM((slots, width), f32),
            pltpu.SemaphoreType.DMA((COPIES,)),
            pltpu.SemaphoreType.DMA((COPIES,)),
            pltpu.SemaphoreType.DMA((COPIES,)),
        ],
        compiler_params=pltpu.CompilerParams(
            collective_id=0, has_side_effects=True, vmem_limit_bytes=VMEM_LIMIT
        ),
        cost_estimate=pl.CostEstimate(
            flops=8 * macs, bytes_accessed=10 * width * hidden, transcendentals=3 * width * hidden
        ),
        name="step",
    )(ids, weight, tokens, cotangent, in_words, out_words, mean, rho, noise)


def grads_kernel(dy_ref, dyr_ref, q_ref, at_ref, bt_ref, gm_ref, gr_ref):
    gm_ref[...] = dot(at_ref[...], dy_ref[...]).astype(gm_ref.dtype)
    gd = dot(bt_ref[...], dyr_ref[...])
    gr_ref[...] = (gd * q_ref[...].astype(jnp.float32)).astype(gr_ref.dtype)


def grads(dy, dyr, q, at, bt, block):
    slots, hidden = dy.shape
    width = q.shape[0]
    weight = pl.BlockSpec((width, block), lambda i: (0, i))
    piece = pl.BlockSpec((slots, block), lambda i: (0, i))
    whole = pl.BlockSpec((width, slots), lambda i: (0, 0))
    out = jax.ShapeDtypeStruct((width, hidden), jnp.bfloat16)
    return pl.pallas_call(
        grads_kernel,
        grid=(hidden // block,),
        in_specs=[piece, piece, weight, whole, whole],
        out_specs=[weight, weight],
        out_shape=[out, out],
        compiler_params=pltpu.CompilerParams(
            dimension_semantics=("arbitrary",), vmem_limit_bytes=40 * 1024 * 1024
        ),
        cost_estimate=pl.CostEstimate(
            flops=4 * slots * width * hidden,
            bytes_accessed=hidden * (6 * width + 4 * slots),
            transcendentals=0,
        ),
        name="grads",
    )(dy, dyr, q, at, bt)


def on_device(
    tokens,
    in_signs,
    out_signs,
    expert_ids,
    route_weight,
    cotangent,
    mean_weight,
    rho_weight,
    noise_weight,
):
    parts = lax.axis_size("dp")
    ranks = lax.axis_size("expert")
    count, width = tokens.shape
    topk = expert_ids.shape[1]
    hidden = mean_weight.shape[2]
    block = cotangent.shape[1]
    capacity = 5 * count * topk // (4 * ranks)
    half = out_signs.shape[1] // 2
    fits = parts == 8 and ranks == RANKS and mean_weight.shape[0] == 1 and topk == 2
    fits = fits and block % LANES == 0 and width % LANES == 0 and count == LANES
    fits = fits and half + in_signs.shape[1] == LANES and half % 8 == 0 and capacity % 16 == 0
    if not fits or hidden % 512:
        return on_device_general(
            tokens,
            in_signs,
            out_signs,
            expert_ids,
            route_weight,
            cotangent,
            mean_weight,
            rho_weight,
            noise_weight,
        )
    hidden_out, fill, g, at, bt, dy, dyr, q = run_step(
        expert_ids.T,
        route_weight.T,
        tokens,
        cotangent,
        in_signs.T,
        out_signs.T,
        mean_weight[0],
        rho_weight[0],
        noise_weight[0],
        capacity,
    )
    pieces = [g[:capacity]]
    for j in range(1, ranks):
        swap = [(z, z ^ j) for z in range(ranks)]
        pieces.append(lax.ppermute(g[j * capacity : (j + 1) * capacity], "expert", swap))
    grad_mean, grad_rho = grads(dy, dyr, q, at, bt, 512)
    g_back = jnp.concatenate(pieces, axis=0)
    grad_tokens = dot(fill, g_back, TN).astype(jnp.bfloat16)
    return (hidden_out, grad_tokens, grad_mean[None], grad_rho[None])


def solution(mesh):
    in_specs = (
        P("expert", "dp"),
        P("expert", "dp"),
        P("expert", None),
        P("expert", None),
        P("expert", None),
        P("expert", "dp"),
        P("expert", "dp", None),
        P("expert", "dp", None),
        P("expert", "dp", None),
    )
    out_specs = (
        P("expert", "dp"),
        P("expert", "dp"),
        P("expert", "dp", None),
        P("expert", "dp", None),
    )
    return jax.shard_map(
        on_device, mesh=mesh, in_specs=in_specs, out_specs=out_specs, check_vma=False
    )
```

```python
import functools

import jax
import jax.numpy as jnp
from jax import lax
from jax.experimental import pallas as pl
from jax.experimental.pallas import tpu as pltpu
from jax.sharding import PartitionSpec as P

def unpack_rows(words):
    shifts = jnp.arange(32, dtype=jnp.int32)
    bits = jnp.bitwise_and(jnp.right_shift(words[..., None], shifts), 1)
    signs = (1 - 2 * bits).astype(jnp.float32)
    return signs.reshape(words.shape[:-1] + (words.shape[-1] * 32,))


def unpack_cols(words):
    shifts = jnp.arange(32, dtype=jnp.int32)
    bits = jnp.bitwise_and(jnp.right_shift(words.T[:, None, :], shifts[None, :, None]), 1)
    signs = (1 - 2 * bits).astype(jnp.float32)
    return signs.reshape(words.shape[1] * 32, words.shape[0])


def block_slots(block_ids, experts, capacity):
    onehot = (block_ids[:, :, None] == jnp.arange(experts, dtype=jnp.int32)).astype(jnp.int32)
    flat = onehot.reshape(-1, experts)
    before = jnp.cumsum(flat, axis=0) - flat
    ranks = jnp.sum(before * flat, axis=1).reshape(block_ids.shape)
    return block_ids * capacity + ranks


def on_device_general(
    tokens,
    in_signs,
    out_signs,
    expert_ids,
    route_weight,
    cotangent,
    mean_weight,
    rho_weight,
    noise_weight,
):
    experts = lax.axis_size("expert") * mean_weight.shape[0]
    token_count = tokens.shape[0]
    topk = expert_ids.shape[1]
    capacity = 5 * token_count * topk // (4 * experts)
    slots = experts * capacity
    width_local = tokens.shape[1]
    sign_words = in_signs.shape[1]
    hidden_local = cotangent.shape[1]
    slot_of = block_slots(expert_ids, experts, capacity)
    match = (slot_of[:, :, None] == jnp.arange(slots, dtype=jnp.int32)).astype(jnp.int32)
    token_rank = jnp.arange(token_count, dtype=jnp.int32)[:, None, None]
    slot_token = jnp.sum(match * token_rank, axis=(0, 1))
    slot_fill = jnp.sum(match, axis=(0, 1))
    slot_weight = jnp.sum(match.astype(jnp.float32) * route_weight[:, :, None], axis=(0, 1))
    words = jnp.concatenate([in_signs, out_signs], axis=1)
    fill_rows = slot_fill.astype(jnp.bfloat16)[:, None]
    send_rows = (jnp.take(tokens, slot_token, axis=0) * fill_rows).reshape(
        experts, capacity, width_local
    )
    send_words = jnp.take(words, slot_token, axis=0).reshape(experts, capacity, words.shape[1])
    recv_rows, recv_words = (
        lax.all_to_all(send_rows, "expert", split_axis=0, concat_axis=0, tiled=True),
        lax.all_to_all(send_words, "expert", split_axis=0, concat_axis=0, tiled=True),
    )
    rows = recv_rows.reshape(slots, width_local)
    recv_words = recv_words.reshape(slots, words.shape[1])
    input_signs = unpack_rows(recv_words[:, :sign_words])
    input_cols = unpack_cols(recv_words[:, :sign_words])
    signed = rows * input_signs.astype(jnp.bfloat16)
    mean_local = mean_weight[0]
    rho_float = rho_weight[0].astype(jnp.float32)
    noise_float = noise_weight[0].astype(jnp.float32)
    delta = (jax.nn.softplus(rho_float) * noise_float).astype(jnp.bfloat16)
    contract = (((0,), (1,)), ((), ()))
    output_cols = unpack_cols(recv_words[:, sign_words:])
    mean_cols = mean_local
    delta_cols = delta
    mean_part = lax.dot_general(mean_cols, rows, contract, preferred_element_type=jnp.float32)
    pert_part = lax.dot_general(delta_cols, signed, contract, preferred_element_type=jnp.float32)
    mean_part, pert_part = (mean_part, pert_part)
    preact = lax.psum_scatter(
        mean_part + output_cols * pert_part, "dp", scatter_dimension=0, tiled=True
    )
    gate = jax.nn.sigmoid(preact)
    hidden_slots = (preact * gate).astype(jnp.bfloat16)
    slope = gate * (1.0 + preact * (1.0 - gate))
    returned = lax.all_to_all(
        hidden_slots.reshape(hidden_local, experts, capacity),
        "expert",
        split_axis=1,
        concat_axis=1,
        tiled=True,
    )
    returned = returned.reshape(hidden_local, slots)
    picked = jnp.take(returned, slot_of, axis=1).astype(jnp.float32)
    hidden_out = jnp.sum(picked * route_weight[None], axis=2).T.astype(jnp.bfloat16)
    upstream = jnp.take(cotangent.T, slot_token, axis=1).astype(jnp.float32) * slot_weight[None, :]
    upstream = upstream.astype(jnp.bfloat16).reshape(hidden_local, experts, capacity)
    arrived = lax.all_to_all(upstream, "expert", split_axis=1, concat_axis=1, tiled=True).reshape(
        hidden_local, slots
    )
    grad_preact = (arrived.astype(jnp.float32) * slope).astype(jnp.bfloat16)
    piece = lax.all_gather(grad_preact, "dp", axis=0, tiled=True)
    piece_signed = piece * output_cols.astype(jnp.bfloat16)
    mean_cols = mean_local
    delta_cols = delta
    grad_rows = jnp.dot(mean_cols, piece, preferred_element_type=jnp.float32)
    grad_signed = jnp.dot(delta_cols, piece_signed, preferred_element_type=jnp.float32)
    mean_block = lax.dot_general(rows, piece, contract, preferred_element_type=jnp.float32)
    delta_block = lax.dot_general(
        signed, piece_signed, contract, preferred_element_type=jnp.float32
    )
    grad_mean_acc = mean_block
    grad_delta_acc = delta_block
    result = (grad_rows, grad_signed, grad_mean_acc, grad_delta_acc)
    grad_rows, grad_signed, grad_mean_acc, grad_delta_acc = result
    slot_grad = (grad_rows + input_cols * grad_signed).astype(jnp.bfloat16)
    back = lax.all_to_all(
        slot_grad.reshape(width_local, experts, capacity),
        "expert",
        split_axis=1,
        concat_axis=1,
        tiled=True,
    )
    back = back.reshape(width_local, slots)
    grad_tokens = jnp.sum(jnp.take(back, slot_of, axis=1).astype(jnp.float32), axis=2).T.astype(
        jnp.bfloat16
    )
    grad_mean = grad_mean_acc.astype(jnp.bfloat16)[None]
    grad_rho = (grad_delta_acc * noise_float * jax.nn.sigmoid(rho_float)).astype(jnp.bfloat16)[None]
    return (hidden_out, grad_tokens, grad_mean, grad_rho)


LANES = 128
VMEM_LIMIT = 40 * 1024 * 1024
RANKS = 4
COPIES = 80
NT = (((1,), (1,)), ((), ()))
TN = (((0,), (0,)), ((), ()))
ORDER = (7, 6, 3, 2, 5, 4, 1, 0)


def dot(a, b, dims=None):
    if dims is None:
        return jnp.dot(a, b, preferred_element_type=jnp.float32)
    return lax.dot_general(a, b, dims, preferred_element_type=jnp.float32)


def total(*terms):
    out = terms[0].astype(jnp.float32)
    for term in terms[1:]:
        out = out + term.astype(jnp.float32)
    return out


def signs_of(words, first, tiles):
    rows = words.shape[0]
    lane = lax.broadcasted_iota(jnp.int32, (rows, LANES), 1)
    shift = lane % 32
    out = []
    for tile in range(tiles):
        at = first + 4 * tile + lane // 32
        picked = jnp.take_along_axis(words, at, axis=1, mode="promise_in_bounds")
        bits = jnp.bitwise_and(jnp.right_shift(picked, shift), 1)
        out.append((1 - 2 * bits).astype(jnp.float32).astype(jnp.bfloat16))
    return jnp.concatenate(out, axis=1) if tiles > 1 else out[0]


def step_kernel(
    ids_ref, weight_ref, tok_ref, cot_ref, inw_ref, outw_ref, mean_hbm, rho_hbm, noise_hbm,
    hid_ref, fill_v, g0_ref, g1_ref, g2_ref, g3_ref, at_ref, bt_ref, dy_v, r_v, q_v,
    mean_v, delta_v, part, rd, cs, land, xs, bs, ss, send_x,
    words_s, words_v, raw, up_s, up_v, h_s, h_v, one_v, plain, signed,
    send_sem, recv_sem, local_sem,
):
    bf16, f32 = jnp.bfloat16, jnp.float32
    me = lax.axis_index("dp")
    mine = lax.axis_index("expert")
    tokens = tok_ref.shape[0]
    width = tok_ref.shape[1]
    block = cot_ref.shape[1]
    cap = up_v.shape[1]
    pair = 2 * cap
    slots = RANKS * cap
    in_words = inw_ref.shape[0]
    half_words = outw_ref.shape[0] // 2
    piece_words = block // 32
    y, x, c = me // 4, (me // 2) % 2, me % 2
    place = lambda dy, dx, dc: ((y + dy) % 2) * 4 + ((x + dx) % 2) * 2 + (c + dc) % 2
    owner = [place(l // 4, (l // 2) % 2, l % 2) for l in range(8)]
    at_x, at_y, at_c = (place(0, 1, 0), mine), (place(1, 0, 0), mine), (place(0, 0, 1), mine)
    zs = [mine, mine + 1 - 2 * (mine % 2), (mine + 2) % 4, 3 - mine]
    at_z = [(me, z) for z in zs]
    count = [0, 0]
    started = []

    def send(src, dst, to):
        n = count[0]
        count[0] += 1
        copy = pltpu.make_async_remote_copy(
            src_ref=src,
            dst_ref=dst,
            send_sem=send_sem.at[n],
            recv_sem=recv_sem.at[n],
            device_id=to,
            device_id_type=pl.DeviceIdType.MESH,
        )
        copy.start()
        started.append(copy)
        return copy

    def local(src, dst):
        n = count[1]
        count[1] += 1
        copy = pltpu.make_async_copy(src, dst, local_sem.at[n])
        copy.start()
        return copy

    cols = [pl.ds(pl.multiple_of(owner[l] * block, LANES), block) for l in range(8)]
    got = {}
    for l in ORDER:
        got[l] = (
            local(rho_hbm.at[:, cols[l]], delta_v.at[l]),
            local(noise_hbm.at[:, cols[l]], q_v.at[l]),
            local(mean_hbm.at[:, cols[l]], mean_v.at[l]),
        )

    barrier = pltpu.get_barrier_semaphore()
    peers = [at_x, at_y, at_c] + at_z[1:]
    for peer in peers:
        pl.semaphore_signal(barrier, inc=1, device_id=peer, device_id_type=pl.DeviceIdType.MESH)

    ids = ids_ref[...]
    weight = weight_ref[...]
    id0, id1 = ids[0:1, :], ids[1:2, :]
    w0, w1 = weight[0:1, :], weight[1:2, :]
    sub16 = lax.broadcasted_iota(jnp.int32, (16, tokens), 0)
    named = jnp.zeros((16, tokens), f32)
    for j in range(RANKS):
        hit = jnp.where(id0 == zs[j], 1.0, 0.0) + jnp.where(id1 == zs[j], 1.0, 0.0)
        named = jnp.where(sub16 == j, jnp.broadcast_to(hit, (16, tokens)), named)
    row_at = lax.broadcasted_iota(jnp.int32, (tokens, tokens), 0)
    col_at = lax.broadcasted_iota(jnp.int32, (tokens, tokens), 1)
    earlier = jnp.where(row_at < col_at, 1.0, 0.0).astype(bf16)
    ranks = dot(named.astype(bf16), earlier)
    slot_at = lax.broadcasted_iota(jnp.int32, (cap, tokens), 0).astype(f32)
    slot_weight = []
    for j in range(RANKS):
        rows = pl.ds(j * cap, cap)
        here = jnp.where(slot_at == ranks[j : j + 1, :], 1.0, 0.0)
        one = here * jnp.where(id0 == zs[j], 1.0, 0.0)
        two = here * jnp.where(id1 == zs[j], 1.0, 0.0)
        one_v[0, rows] = one.astype(bf16)
        one_v[1, rows] = two.astype(bf16)
        fill_v[rows] = (one + two).astype(bf16)
        slot_weight.append(jnp.sum(one * w0 + two * w1, axis=1, keepdims=True))
    fill = fill_v[...]
    taken = dot(fill, tok_ref[...]).astype(bf16)
    xs[pl.ds(0, cap)] = taken[:cap]
    send_x[...] = taken
    words_s[pl.ds(0, half_words)] = outw_ref[pl.ds(pl.multiple_of(c * half_words, 8), half_words)]
    words_s[pl.ds(half_words, in_words)] = inw_ref[...]
    words = words_s[...]
    gathered = None
    for k in range(4):
        plane = jnp.bitwise_and(jnp.right_shift(words, 8 * k), 255).astype(f32).astype(bf16)
        got_plane = jnp.left_shift(dot(fill, plane, NT).astype(jnp.int32), 8 * k)
        gathered = got_plane if k == 0 else jnp.bitwise_or(gathered, got_plane)
    raw[...] = gathered
    words_v[c, pl.ds(0, cap)] = gathered[:cap]

    block_rows = [pl.ds(j * cap, cap) for j in range(RANKS)]
    pair_rows = [pl.ds(0, pair), pl.ds(pair, pair)]
    x_in, w_in, w_swap, up_in = {}, {}, {}, {}

    def send_rows(j):
        x_in[j] = send(send_x.at[block_rows[j]], xs.at[block_rows[j]], at_z[j])

    def send_words(j):
        w_in[j] = send(raw.at[block_rows[j]], words_v.at[c, block_rows[j]], at_z[j])

    def swap_words(j):
        here = words_v.at[c, block_rows[j]]
        w_swap[j] = send(here, here, at_c)

    def make_delta(l):
        got[l][0].wait()
        got[l][1].wait()

        @pl.loop(0, width // 32)
        def _(i):
            rows = pl.ds(pl.multiple_of(i * 32, 32), 32)
            rho = delta_v[l, rows].astype(f32)
            noise = q_v[l, rows].astype(f32)
            soft = jnp.log(1.0 + jnp.exp(rho))
            delta_v[l, rows] = (soft * noise).astype(bf16)
            q_v[l, rows] = (jnp.exp(rho - soft) * noise).astype(bf16)

    make_delta(ORDER[0])
    pl.semaphore_wait(barrier, len(peers))
    send_words(1)
    send_rows(1)
    send_words(2)
    send_words(3)
    send_rows(2)
    send_rows(3)
    swap_words(0)
    make_delta(ORDER[1])
    up = dot(fill, cot_ref[...])
    for j in range(RANKS):
        mixed = (up[j * cap : (j + 1) * cap] * slot_weight[j]).astype(bf16)
        if j == 0:
            up_v[0] = mixed
        else:
            up_s[j] = mixed
    for j in range(1, RANKS):
        up_in[j] = send(up_s.at[j], up_v.at[j], at_z[j])
    make_delta(ORDER[2])
    w_in[1].wait_recv()
    swap_words(1)
    make_delta(ORDER[3])
    made = set(ORDER[:4])

    def arrive(p):
        if p == 1:
            for j in (2, 3):
                w_in[j].wait_recv()
                swap_words(j)
        for j in (1,) if p == 0 else (2, 3):
            x_in[j].wait_recv()
        rows = pair_rows[p]
        signs = signs_of(words_v[c, rows], half_words, width // LANES)
        ss[rows] = signs
        bs[rows] = xs[rows] * signs
        for j in (2 * p, 2 * p + 1):
            w_swap[j].wait_recv()

    def forward(p, l):
        rows = pair_rows[p]
        if l not in made:
            make_delta(l)
            made.add(l)
        if p == 0:
            got[l][2].wait()
        one = dot(xs[rows], mean_v[l])
        two = dot(bs[rows], delta_v[l])
        signs = signs_of(
            words_v[owner[l] // 4, rows], (owner[l] % 4) * piece_words, block // LANES
        )
        r_v[l, rows] = signs
        part[l, rows] = (one + signs.astype(f32) * two).astype(bf16)

    core, sent = {}, {}

    def to_core(p, k):
        rows = pair_rows[p]
        core[p, k] = send(part.at[2 * k + 1, rows], rd.at[k, rows], at_c)

    def hop(p, k, which, name, to, extra=None):
        rows = block_rows[2 * p + which]
        terms = [part[2 * k, rows], rd[k, rows]]
        if extra is not None:
            terms.append(land[p, extra])
        cs[k, rows] = total(*terms).astype(bf16)
        sent[p, name] = send(cs.at[k, rows], land.at[p, name], to)

    D_X, D_Y, N_X, N_Y, L_Y, L_X = range(6)

    def reduce_first(p, early, late):
        forward(p, 7)
        to_core(p, 3)
        forward(p, 6)
        core[p, 3].wait_recv()
        hop(p, 3, 0, D_X, at_x)
        hop(p, 3, 1, D_Y, at_y)
        forward(p, 3)
        to_core(p, 1)
        forward(p, 2)
        core[p, 1].wait_recv()
        hop(p, 1, 0, N_X, at_x)
        forward(p, 5)
        to_core(p, 2)
        forward(p, 4)
        core[p, 2].wait_recv()
        hop(p, 2, 1, N_Y, at_y)
        early()
        forward(p, 1)
        to_core(p, 0)
        reduce_last(p)
        late()
        forward(p, 0)
        core[p, 0].wait_recv()

    def reduce_last(p):
        sent[p, D_X].wait_recv()
        hop(p, 2, 0, L_Y, at_y, D_X)
        sent[p, D_Y].wait_recv()
        hop(p, 1, 1, L_X, at_x, D_Y)

    spread, h_in = {}, {}

    def pass_on(p, which, l, to_l, to, name):
        rows = block_rows[2 * p + which]
        spread[p, name] = send(dy_v.at[l, rows], dy_v.at[to_l, rows], to)

    def activate(p, which):
        j = 2 * p + which
        rows = block_rows[j]
        if j > 0:
            up_in[j].wait_recv()
        near, last = (N_X, L_Y) if which == 0 else (N_Y, L_X)
        sent[p, near].wait_recv()
        sent[p, last].wait_recv()
        preact = total(part[0, rows], rd[0, rows], land[p, near], land[p, last])
        gate = 1.0 / (1.0 + jnp.exp(-preact))
        hidden = (preact * gate).astype(bf16)
        slope = gate * (1.0 + preact * (1.0 - gate))
        dy_v[0, rows] = (up_v[j].astype(f32) * slope).astype(bf16)
        if j == 0:
            h_v[0] = hidden
        else:
            h_s[j] = hidden

    def gather_first(p):
        activate(p, 0)
        pass_on(p, 0, 0, 4, at_y, "y1")
        pass_on(p, 0, 0, 1, at_c, "c0")
        activate(p, 1)
        pass_on(p, 1, 0, 2, at_x, "x1")
        pass_on(p, 1, 0, 1, at_c, "c1")
        for j in (2 * p, 2 * p + 1):
            if j > 0:
                h_in[j] = send(h_s.at[j], h_v.at[j], at_z[j])

    def gather_second(p):
        pass_on(p, 0, 0, 2, at_x, "x2")
        pass_on(p, 1, 0, 4, at_y, "y2")

    def gather_relay(p):
        spread[p, "y1"].wait_recv()
        pass_on(p, 0, 4, 6, at_x, "x3")
        pass_on(p, 0, 4, 5, at_c, "c2")
        spread[p, "x1"].wait_recv()
        pass_on(p, 1, 2, 6, at_y, "y3")
        pass_on(p, 1, 2, 3, at_c, "c3")

    def gather_near(p):
        spread[p, "x2"].wait_recv()
        pass_on(p, 0, 2, 3, at_c, "c4")
        spread[p, "y2"].wait_recv()
        pass_on(p, 1, 4, 5, at_c, "c5")

    def gather_last(p):
        spread[p, "x3"].wait_recv()
        pass_on(p, 0, 6, 7, at_c, "c6")
        spread[p, "y3"].wait_recv()
        pass_on(p, 1, 6, 7, at_c, "c7")

    first_back = {0: True, 1: True}

    def back(p, l, waits=()):
        for name in waits:
            spread[p, name].wait_recv()
        rows = pair_rows[p]
        dy = dy_v[l, rows]
        dyr = dy * r_v[l, rows]
        r_v[l, rows] = dyr
        one = dot(dy, mean_v[l], NT)
        two = dot(dyr, delta_v[l], NT)
        if first_back[p]:
            plain[rows] = one
            signed[rows] = two
            first_back[p] = False
        else:
            plain[rows] += one
            signed[rows] += two

    arrive(0)
    reduce_first(0, lambda: None, lambda: None)
    arrive(1)
    reduce_first(1, lambda: gather_first(0), lambda: gather_second(0))
    at_ref[...] = xs[...].T
    bt_ref[...] = bs[...].T
    back(0, 0)
    back(0, 1, ("c0", "c1"))
    gather_relay(0)
    gather_first(1)
    gather_second(1)
    gather_near(0)
    back(0, 2)
    back(0, 4)
    back(0, 3, ("c3", "c4"))
    back(0, 5, ("c2", "c5"))
    back(1, 0)
    back(1, 1, ("c0", "c1"))
    gather_last(0)
    back(0, 6)
    back(0, 7, ("c6", "c7"))
    gather_relay(1)
    gather_near(1)
    back(1, 2)
    back(1, 4)
    back(1, 3, ("c3", "c4"))
    back(1, 5, ("c2", "c5"))
    for j in range(1, RANKS):
        h_in[j].wait_recv()
    out = None
    for k, w in enumerate((w0, w1)):
        column = jnp.sum(jnp.where(row_at == col_at, w, 0.0), axis=1, keepdims=True)
        picked = None
        for j in range(RANKS):
            one = dot(one_v[k, block_rows[j]], h_v[j], TN)
            picked = one if picked is None else picked + one
        picked = picked * column
        out = picked if out is None else out + picked
    hid_ref[...] = out.astype(bf16)
    gather_last(1)
    back(1, 6)
    back(1, 7, ("c6", "c7"))
    for j, g_ref in enumerate((g0_ref, g1_ref, g2_ref, g3_ref)):
        rows = block_rows[j]
        g_ref[...] = (plain[rows] + ss[rows].astype(f32) * signed[rows]).astype(bf16)
    for copy in started:
        copy.wait_send()


def run_step(ids, weight, tokens, cotangent, in_words, out_words, mean, rho, noise, cap):
    bf16, f32 = jnp.bfloat16, jnp.float32
    width, hidden = mean.shape
    count = tokens.shape[0]
    block = cotangent.shape[1]
    slots = RANKS * cap
    vmem = pl.BlockSpec(memory_space=pltpu.VMEM)
    hbm = pl.BlockSpec(memory_space=pltpu.MemorySpace.HBM)
    shape = jax.ShapeDtypeStruct
    weights = pltpu.VMEM((8, width, block), bf16)
    piece = pltpu.VMEM((8, slots, block), bf16)
    four = pltpu.VMEM((4, slots, block), bf16)
    small = pltpu.VMEM((slots, width), bf16)
    per = pltpu.VMEM((RANKS, cap, block), bf16)
    macs = slots * width * hidden
    return pl.pallas_call(
        step_kernel,
        in_specs=[vmem] * 6 + [hbm] * 3,
        out_specs=[vmem] * 11,
        out_shape=[
            pltpu.VMEM((count, block), bf16),
            shape((slots, count), bf16),
            *[shape((cap, width), bf16)] * RANKS,
            pltpu.VMEM((width, slots), bf16),
            pltpu.VMEM((width, slots), bf16),
            piece,
            piece,
            weights,
        ],
        scratch_shapes=[
            weights, weights, piece, four, four,
            pltpu.VMEM((2, 6, cap, block), bf16),
            small, small, small, small,
            pltpu.VMEM((LANES, count), jnp.int32),
            pltpu.VMEM((2, slots, LANES), jnp.int32),
            pltpu.VMEM((slots, LANES), jnp.int32),
            per, per, per, per,
            pltpu.VMEM((2, slots, count), bf16),
            pltpu.VMEM((slots, width), f32),
            pltpu.VMEM((slots, width), f32),
            pltpu.SemaphoreType.DMA((COPIES,)),
            pltpu.SemaphoreType.DMA((COPIES,)),
            pltpu.SemaphoreType.DMA((COPIES,)),
        ],
        compiler_params=pltpu.CompilerParams(
            collective_id=0, has_side_effects=True, vmem_limit_bytes=VMEM_LIMIT
        ),
        cost_estimate=pl.CostEstimate(
            flops=8 * macs, bytes_accessed=10 * width * hidden, transcendentals=3 * width * hidden
        ),
        name="step",
    )(ids, weight, tokens, cotangent, in_words, out_words, mean, rho, noise)


def grads_kernel(hid_ref, dy_ref, dyr_ref, q_ref, at_ref, bt_ref, hid_out, gm_out, gr_out, gm, gr, sem):
    me = lax.axis_index("dp")
    block = dy_ref.shape[2]
    y, x, c = me // 4, (me // 2) % 2, me % 2
    first = pltpu.make_async_copy(hid_ref, hid_out, sem.at[4])
    first.start()
    waiting = [None, None]
    for l in range(8):
        slot = l % 2
        owner = ((y + l // 4) % 2) * 4 + ((x + (l // 2) % 2) % 2) * 2 + (c + l) % 2
        cols = pl.ds(pl.multiple_of(owner * block, LANES), block)
        if waiting[slot] is not None:
            waiting[slot][0].wait()
        gm[slot] = dot(at_ref[...], dy_ref[l]).astype(gm.dtype)
        one = pltpu.make_async_copy(gm.at[slot], gm_out.at[:, cols], sem.at[2 * slot])
        one.start()
        if waiting[slot] is not None:
            waiting[slot][1].wait()
        gd = dot(bt_ref[...], dyr_ref[l])
        gr[slot] = (gd * q_ref[l].astype(jnp.float32)).astype(gr.dtype)
        two = pltpu.make_async_copy(gr.at[slot], gr_out.at[:, cols], sem.at[2 * slot + 1])
        two.start()
        waiting[slot] = (one, two)
    for pair in waiting:
        for copy in pair:
            copy.wait()
    first.wait()


def grads(hid, dy, dyr, q, at, bt):
    parts, slots, block = dy.shape
    width = q.shape[1]
    vmem = pl.BlockSpec(memory_space=pltpu.VMEM)
    hbm = pl.BlockSpec(memory_space=pltpu.MemorySpace.HBM)
    out = jax.ShapeDtypeStruct((width, parts * block), jnp.bfloat16)
    stage = pltpu.VMEM((2, width, block), jnp.bfloat16)
    return pl.pallas_call(
        grads_kernel,
        in_specs=[vmem] * 6,
        out_specs=[hbm] * 3,
        out_shape=[jax.ShapeDtypeStruct(hid.shape, hid.dtype), out, out],
        scratch_shapes=[stage, stage, pltpu.SemaphoreType.DMA((5,))],
        compiler_params=pltpu.CompilerParams(vmem_limit_bytes=16 * 1024 * 1024),
        cost_estimate=pl.CostEstimate(
            flops=4 * slots * width * parts * block,
            bytes_accessed=6 * width * parts * block,
            transcendentals=0,
        ),
        name="grads",
    )(hid, dy, dyr, q, at, bt)


def on_device(
    tokens,
    in_signs,
    out_signs,
    expert_ids,
    route_weight,
    cotangent,
    mean_weight,
    rho_weight,
    noise_weight,
):
    parts = lax.axis_size("dp")
    ranks = lax.axis_size("expert")
    count, width = tokens.shape
    topk = expert_ids.shape[1]
    hidden = mean_weight.shape[2]
    block = cotangent.shape[1]
    capacity = 5 * count * topk // (4 * ranks)
    half = out_signs.shape[1] // 2
    fits = parts == 8 and ranks == RANKS and mean_weight.shape[0] == 1 and topk == 2
    fits = fits and block % LANES == 0 and width % LANES == 0 and count == LANES
    fits = fits and half + in_signs.shape[1] == LANES and half % 8 == 0 and capacity % 16 == 0
    if not fits or hidden % 512:
        return on_device_general(
            tokens,
            in_signs,
            out_signs,
            expert_ids,
            route_weight,
            cotangent,
            mean_weight,
            rho_weight,
            noise_weight,
        )
    hidden_out, fill, g0, g1, g2, g3, at, bt, dy, dyr, q = run_step(
        expert_ids.T,
        route_weight.T,
        tokens,
        cotangent,
        in_signs.T,
        out_signs.T,
        mean_weight[0],
        rho_weight[0],
        noise_weight[0],
        capacity,
    )
    pieces = [g0]
    for j, piece in enumerate((g1, g2, g3), 1):
        pieces.append(lax.ppermute(piece, "expert", [(z, z ^ j) for z in range(ranks)]))
    hidden_out, grad_mean, grad_rho = grads(hidden_out, dy, dyr, q, at, bt)
    grad_tokens = dot(fill, jnp.concatenate(pieces, axis=0), TN).astype(jnp.bfloat16)
    return (hidden_out, grad_tokens, grad_mean[None], grad_rho[None])


def solution(mesh):
    in_specs = (
        P("expert", "dp"),
        P("expert", "dp"),
        P("expert", None),
        P("expert", None),
        P("expert", None),
        P("expert", "dp"),
        P("expert", "dp", None),
        P("expert", "dp", None),
        P("expert", "dp", None),
    )
    out_specs = (
        P("expert", "dp"),
        P("expert", "dp"),
        P("expert", "dp", None),
        P("expert", "dp", None),
    )
    return jax.shard_map(
        on_device, mesh=mesh, in_specs=in_specs, out_specs=out_specs, check_vma=False
    )
```

```python
import functools

import jax
import jax.numpy as jnp
from jax import lax
from jax.experimental import pallas as pl
from jax.experimental.pallas import tpu as pltpu
from jax.sharding import PartitionSpec as P

def unpack_rows(words):
    shifts = jnp.arange(32, dtype=jnp.int32)
    bits = jnp.bitwise_and(jnp.right_shift(words[..., None], shifts), 1)
    signs = (1 - 2 * bits).astype(jnp.float32)
    return signs.reshape(words.shape[:-1] + (words.shape[-1] * 32,))


def unpack_cols(words):
    shifts = jnp.arange(32, dtype=jnp.int32)
    bits = jnp.bitwise_and(jnp.right_shift(words.T[:, None, :], shifts[None, :, None]), 1)
    signs = (1 - 2 * bits).astype(jnp.float32)
    return signs.reshape(words.shape[1] * 32, words.shape[0])


def block_slots(block_ids, experts, capacity):
    onehot = (block_ids[:, :, None] == jnp.arange(experts, dtype=jnp.int32)).astype(jnp.int32)
    flat = onehot.reshape(-1, experts)
    before = jnp.cumsum(flat, axis=0) - flat
    ranks = jnp.sum(before * flat, axis=1).reshape(block_ids.shape)
    return block_ids * capacity + ranks


def on_device_general(
    tokens,
    in_signs,
    out_signs,
    expert_ids,
    route_weight,
    cotangent,
    mean_weight,
    rho_weight,
    noise_weight,
):
    experts = lax.axis_size("expert") * mean_weight.shape[0]
    token_count = tokens.shape[0]
    topk = expert_ids.shape[1]
    capacity = 5 * token_count * topk // (4 * experts)
    slots = experts * capacity
    width_local = tokens.shape[1]
    sign_words = in_signs.shape[1]
    hidden_local = cotangent.shape[1]
    slot_of = block_slots(expert_ids, experts, capacity)
    match = (slot_of[:, :, None] == jnp.arange(slots, dtype=jnp.int32)).astype(jnp.int32)
    token_rank = jnp.arange(token_count, dtype=jnp.int32)[:, None, None]
    slot_token = jnp.sum(match * token_rank, axis=(0, 1))
    slot_fill = jnp.sum(match, axis=(0, 1))
    slot_weight = jnp.sum(match.astype(jnp.float32) * route_weight[:, :, None], axis=(0, 1))
    words = jnp.concatenate([in_signs, out_signs], axis=1)
    fill_rows = slot_fill.astype(jnp.bfloat16)[:, None]
    send_rows = (jnp.take(tokens, slot_token, axis=0) * fill_rows).reshape(
        experts, capacity, width_local
    )
    send_words = jnp.take(words, slot_token, axis=0).reshape(experts, capacity, words.shape[1])
    recv_rows, recv_words = (
        lax.all_to_all(send_rows, "expert", split_axis=0, concat_axis=0, tiled=True),
        lax.all_to_all(send_words, "expert", split_axis=0, concat_axis=0, tiled=True),
    )
    rows = recv_rows.reshape(slots, width_local)
    recv_words = recv_words.reshape(slots, words.shape[1])
    input_signs = unpack_rows(recv_words[:, :sign_words])
    input_cols = unpack_cols(recv_words[:, :sign_words])
    signed = rows * input_signs.astype(jnp.bfloat16)
    mean_local = mean_weight[0]
    rho_float = rho_weight[0].astype(jnp.float32)
    noise_float = noise_weight[0].astype(jnp.float32)
    delta = (jax.nn.softplus(rho_float) * noise_float).astype(jnp.bfloat16)
    contract = (((0,), (1,)), ((), ()))
    output_cols = unpack_cols(recv_words[:, sign_words:])
    mean_cols = mean_local
    delta_cols = delta
    mean_part = lax.dot_general(mean_cols, rows, contract, preferred_element_type=jnp.float32)
    pert_part = lax.dot_general(delta_cols, signed, contract, preferred_element_type=jnp.float32)
    mean_part, pert_part = (mean_part, pert_part)
    preact = lax.psum_scatter(
        mean_part + output_cols * pert_part, "dp", scatter_dimension=0, tiled=True
    )
    gate = jax.nn.sigmoid(preact)
    hidden_slots = (preact * gate).astype(jnp.bfloat16)
    slope = gate * (1.0 + preact * (1.0 - gate))
    returned = lax.all_to_all(
        hidden_slots.reshape(hidden_local, experts, capacity),
        "expert",
        split_axis=1,
        concat_axis=1,
        tiled=True,
    )
    returned = returned.reshape(hidden_local, slots)
    picked = jnp.take(returned, slot_of, axis=1).astype(jnp.float32)
    hidden_out = jnp.sum(picked * route_weight[None], axis=2).T.astype(jnp.bfloat16)
    upstream = jnp.take(cotangent.T, slot_token, axis=1).astype(jnp.float32) * slot_weight[None, :]
    upstream = upstream.astype(jnp.bfloat16).reshape(hidden_local, experts, capacity)
    arrived = lax.all_to_all(upstream, "expert", split_axis=1, concat_axis=1, tiled=True).reshape(
        hidden_local, slots
    )
    grad_preact = (arrived.astype(jnp.float32) * slope).astype(jnp.bfloat16)
    piece = lax.all_gather(grad_preact, "dp", axis=0, tiled=True)
    piece_signed = piece * output_cols.astype(jnp.bfloat16)
    mean_cols = mean_local
    delta_cols = delta
    grad_rows = jnp.dot(mean_cols, piece, preferred_element_type=jnp.float32)
    grad_signed = jnp.dot(delta_cols, piece_signed, preferred_element_type=jnp.float32)
    mean_block = lax.dot_general(rows, piece, contract, preferred_element_type=jnp.float32)
    delta_block = lax.dot_general(
        signed, piece_signed, contract, preferred_element_type=jnp.float32
    )
    grad_mean_acc = mean_block
    grad_delta_acc = delta_block
    result = (grad_rows, grad_signed, grad_mean_acc, grad_delta_acc)
    grad_rows, grad_signed, grad_mean_acc, grad_delta_acc = result
    slot_grad = (grad_rows + input_cols * grad_signed).astype(jnp.bfloat16)
    back = lax.all_to_all(
        slot_grad.reshape(width_local, experts, capacity),
        "expert",
        split_axis=1,
        concat_axis=1,
        tiled=True,
    )
    back = back.reshape(width_local, slots)
    grad_tokens = jnp.sum(jnp.take(back, slot_of, axis=1).astype(jnp.float32), axis=2).T.astype(
        jnp.bfloat16
    )
    grad_mean = grad_mean_acc.astype(jnp.bfloat16)[None]
    grad_rho = (grad_delta_acc * noise_float * jax.nn.sigmoid(rho_float)).astype(jnp.bfloat16)[None]
    return (hidden_out, grad_tokens, grad_mean, grad_rho)


LANES = 128
VMEM_LIMIT = 34 * 1024 * 1024
RANKS = 4
COPIES = 80
NT = (((1,), (1,)), ((), ()))
TN = (((0,), (0,)), ((), ()))
ORDER = (7, 6, 3, 2, 5, 4, 1, 0)
DONE = (0, 1, 2)
LEFT = (3, 4, 5, 6, 7)


def dot(a, b, dims=None):
    if dims is None:
        return jnp.dot(a, b, preferred_element_type=jnp.float32)
    return lax.dot_general(a, b, dims, preferred_element_type=jnp.float32)


def total(*terms):
    out = terms[0].astype(jnp.float32)
    for term in terms[1:]:
        out = out + term.astype(jnp.float32)
    return out


def signs_of(words, first, tiles):
    rows = words.shape[0]
    lane = lax.broadcasted_iota(jnp.int32, (rows, LANES), 1)
    shift = lane % 32
    out = []
    for tile in range(tiles):
        at = first + 4 * tile + lane // 32
        picked = jnp.take_along_axis(words, at, axis=1, mode="promise_in_bounds")
        bits = jnp.bitwise_and(jnp.right_shift(picked, shift), 1)
        out.append((1 - 2 * bits).astype(jnp.float32).astype(jnp.bfloat16))
    return jnp.concatenate(out, axis=1) if tiles > 1 else out[0]


def step_kernel(
    ids_ref, weight_ref, tok_ref, cot_ref, inw_ref, outw_ref, mean_hbm, rho_hbm, noise_hbm,
    hid_ref, fill_v, g0_ref, g1_ref, g2_ref, g3_ref, at_ref, bt_ref, dy_v, r_v, q_v, mean_v,
    delta_v, part, rd, land, xs, bs, ss, send_x,
    words_s, words_v, raw, up_s, up_v, h_s, h_v, one_v, plain, signed, g_s,
    send_sem, recv_sem, local_sem,
):
    bf16, f32 = jnp.bfloat16, jnp.float32
    me = lax.axis_index("dp")
    mine = lax.axis_index("expert")
    tokens = tok_ref.shape[0]
    width = tok_ref.shape[1]
    block = cot_ref.shape[1]
    cap = up_v.shape[1]
    slots = RANKS * cap
    in_words = inw_ref.shape[0]
    half_words = outw_ref.shape[0] // 2
    piece_words = block // 32
    y, x, c = me // 4, (me // 2) % 2, me % 2
    place = lambda dy, dx, dc: ((y + dy) % 2) * 4 + ((x + dx) % 2) * 2 + (c + dc) % 2
    owner = [place(l // 4, (l // 2) % 2, l % 2) for l in range(8)]
    at_x, at_y, at_c = (place(0, 1, 0), mine), (place(1, 0, 0), mine), (place(0, 0, 1), mine)
    zs = [mine, mine + 1 - 2 * (mine % 2), (mine + 2) % 4, 3 - mine]
    at_z = [(me, z) for z in zs]
    count = [0, 0]
    started = []

    def send(src, dst, to):
        n = count[0]
        count[0] += 1
        copy = pltpu.make_async_remote_copy(
            src_ref=src,
            dst_ref=dst,
            send_sem=send_sem.at[n],
            recv_sem=recv_sem.at[n],
            device_id=to,
            device_id_type=pl.DeviceIdType.MESH,
        )
        copy.start()
        started.append(copy)
        return copy

    def local(src, dst):
        n = count[1]
        count[1] += 1
        copy = pltpu.make_async_copy(src, dst, local_sem.at[n])
        copy.start()
        return copy

    cols = [pl.ds(pl.multiple_of(owner[l] * block, LANES), block) for l in range(8)]
    got = {}
    for l in ORDER:
        got[l] = (
            local(rho_hbm.at[:, cols[l]], delta_v.at[l]),
            local(noise_hbm.at[:, cols[l]], q_v.at[l]),
            local(mean_hbm.at[:, cols[l]], mean_v.at[l]),
        )

    barrier = pltpu.get_barrier_semaphore()
    peers = [at_x, at_y, at_c] + at_z[1:]
    for peer in peers:
        pl.semaphore_signal(barrier, inc=1, device_id=peer, device_id_type=pl.DeviceIdType.MESH)

    ids = ids_ref[...]
    weight = weight_ref[...]
    id0, id1 = ids[0:1, :], ids[1:2, :]
    w0, w1 = weight[0:1, :], weight[1:2, :]
    sub16 = lax.broadcasted_iota(jnp.int32, (16, tokens), 0)
    named = jnp.zeros((16, tokens), f32)
    for j in range(RANKS):
        hit = jnp.where(id0 == zs[j], 1.0, 0.0) + jnp.where(id1 == zs[j], 1.0, 0.0)
        named = jnp.where(sub16 == j, jnp.broadcast_to(hit, (16, tokens)), named)
    row_at = lax.broadcasted_iota(jnp.int32, (tokens, tokens), 0)
    col_at = lax.broadcasted_iota(jnp.int32, (tokens, tokens), 1)
    earlier = jnp.where(row_at < col_at, 1.0, 0.0).astype(bf16)
    ranks = dot(named.astype(bf16), earlier)
    slot_at = lax.broadcasted_iota(jnp.int32, (cap, tokens), 0).astype(f32)
    slot_weight = []
    for j in range(RANKS):
        rows = pl.ds(j * cap, cap)
        here = jnp.where(slot_at == ranks[j : j + 1, :], 1.0, 0.0)
        one = here * jnp.where(id0 == zs[j], 1.0, 0.0)
        two = here * jnp.where(id1 == zs[j], 1.0, 0.0)
        one_v[0, rows] = one.astype(bf16)
        one_v[1, rows] = two.astype(bf16)
        fill_v[rows] = (one + two).astype(bf16)
        slot_weight.append(jnp.sum(one * w0 + two * w1, axis=1, keepdims=True))
    fill = fill_v[...]
    taken = dot(fill, tok_ref[...]).astype(bf16)
    xs[pl.ds(0, cap)] = taken[:cap]
    send_x[...] = taken
    words_s[pl.ds(0, half_words)] = outw_ref[pl.ds(pl.multiple_of(c * half_words, 8), half_words)]
    words_s[pl.ds(half_words, in_words)] = inw_ref[...]
    words = words_s[...]
    gathered = None
    for k in range(4):
        plane = jnp.bitwise_and(jnp.right_shift(words, 8 * k), 255).astype(f32).astype(bf16)
        got_plane = jnp.left_shift(dot(fill, plane, NT).astype(jnp.int32), 8 * k)
        gathered = got_plane if k == 0 else jnp.bitwise_or(gathered, got_plane)
    raw[...] = gathered
    words_v[c, pl.ds(0, cap)] = gathered[:cap]

    block_rows = [pl.ds(j * cap, cap) for j in range(RANKS)]
    span = lambda first, n: pl.ds(first * cap, n * cap)
    x_in, w_in, w_swap, up_in = {}, {}, {}, {}

    def send_rows(j):
        x_in[j] = send(send_x.at[block_rows[j]], xs.at[block_rows[j]], at_z[j])

    def send_words(j):
        w_in[j] = send(raw.at[block_rows[j]], words_v.at[c, block_rows[j]], at_z[j])

    def swap_words(j):
        here = words_v.at[c, block_rows[j]]
        w_swap[j] = send(here, here, at_c)

    def make_delta(l):
        got[l][0].wait()
        got[l][1].wait()

        @pl.loop(0, width // LANES)
        def _(i):
            rows = pl.ds(pl.multiple_of(i * LANES, LANES), LANES)
            noise = q_v[l, rows].astype(f32)
            grown = jnp.exp(delta_v[l, rows].astype(f32))
            more = 1.0 + grown
            delta_v[l, rows] = (jnp.log(more) * noise).astype(bf16)
            q_v[l, rows] = (grown / more * noise).astype(bf16)

    made, loaded = set(), set()

    def make(l):
        if l not in made:
            make_delta(l)
            made.add(l)

    def swap_in(j):
        w_in[j].wait_recv()
        swap_words(j)

    def arrive(first, n):
        for j in range(first, first + n):
            if j > 0:
                x_in[j].wait_recv()
        rows = span(first, n)
        signs = signs_of(words_v[c, rows], half_words, width // LANES)
        ss[rows] = signs
        bs[rows] = xs[rows] * signs
        for j in range(first, first + n):
            w_swap[j].wait_recv()

    core, sent = {}, {}

    def forward(first, n, l):
        make(l)
        if l not in loaded:
            got[l][2].wait()
            loaded.add(l)
        rows = span(first, n)
        one = dot(xs[rows], mean_v[l])
        two = dot(bs[rows], delta_v[l])
        signs = signs_of(
            words_v[owner[l] // 4, rows], (owner[l] % 4) * piece_words, block // LANES
        )
        r_v[l, rows] = signs
        part[l, rows] = (one + signs.astype(f32) * two).astype(bf16)
        if l % 2:
            core[first, l // 2] = send(part.at[l, rows], rd.at[l // 2, rows], at_c)

    D, N, L = range(3)

    def hop(j, k, name, to, extra=None):
        rows = block_rows[j]
        terms = [part[2 * k, rows], rd[k, rows]]
        if extra is not None:
            terms.append(land[j, extra])
        part[2 * k, rows] = total(*terms).astype(bf16)
        sent[j, name] = send(part.at[2 * k, rows], land.at[j, name], to)

    def d_hop(j):
        hop(j, 3, D, (at_x, at_y)[j % 2])

    def n_hop(j):
        hop(j, 1 + j % 2, N, (at_x, at_y)[j % 2])

    def l_hop(j):
        sent[j, D].wait_recv()
        hop(j, 2 - j % 2, L, (at_y, at_x)[j % 2], D)

    spread, h_in = {}, {}

    def pass_on(j, l, to_l, to, name):
        rows = block_rows[j]
        spread[j, name] = send(dy_v.at[l, rows], dy_v.at[to_l, rows], to)

    def activate(j):
        rows = block_rows[j]
        if j > 0:
            up_in[j].wait_recv()
        sent[j, N].wait_recv()
        sent[j, L].wait_recv()
        preact = total(part[0, rows], rd[0, rows], land[j, N], land[j, L])
        gate = 1.0 / (1.0 + jnp.exp(-preact))
        hidden = (preact * gate).astype(bf16)
        slope = gate * (1.0 + preact * (1.0 - gate))
        dy_v[0, rows] = (up_v[j].astype(f32) * slope).astype(bf16)
        if j == 0:
            h_v[0] = hidden
        else:
            h_s[j] = hidden

    def g_first(j):
        activate(j)
        pass_on(j, 0, (4, 2)[j % 2], (at_y, at_x)[j % 2], "first")
        pass_on(j, 0, 1, at_c, "c0")
        if j > 0:
            h_in[j] = send(h_s.at[j], h_v.at[j], at_z[j])

    def g_second(j):
        pass_on(j, 0, (2, 4)[j % 2], (at_x, at_y)[j % 2], "second")

    def g_relay(j):
        spread[j, "first"].wait_recv()
        l = (4, 2)[j % 2]
        pass_on(j, l, 6, (at_x, at_y)[j % 2], "relay")
        pass_on(j, l, l + 1, at_c, "c%d" % l)

    def g_near(j):
        spread[j, "second"].wait_recv()
        l = (2, 4)[j % 2]
        pass_on(j, l, l + 1, at_c, "c%d" % l)

    def g_last(j):
        spread[j, "relay"].wait_recv()
        pass_on(j, 6, 7, at_c, "c6")

    begun = set()

    def back(p, l):
        if l % 2:
            for j in (2 * p, 2 * p + 1):
                spread[j, "c%d" % (l - 1)].wait_recv()
        rows = span(2 * p, 2)
        dy = dy_v[l, rows]
        dyr = dy * r_v[l, rows]
        r_v[l, rows] = dyr
        one = dot(dy, mean_v[l], NT)
        two = dot(dyr, delta_v[l], NT)
        if p not in begun:
            plain[rows] = one
            signed[rows] = two
            begun.add(p)
        else:
            plain[rows] += one
            signed[rows] += two

    def grad(l):
        mean_v[l] = dot(at_ref[...], dy_v[l]).astype(bf16)
        q_v[l] = (dot(bt_ref[...], r_v[l]) * q_v[l].astype(f32)).astype(bf16)

    def g_make(j, ref):
        rows = block_rows[j]
        ref[...] = (plain[rows] + ss[rows].astype(f32) * signed[rows]).astype(bf16)

    make(7)
    pl.semaphore_wait(barrier, len(peers))
    send_words(1)
    send_rows(1)
    send_words(2)
    send_words(3)
    send_rows(2)
    send_rows(3)
    swap_words(0)
    make(6)
    arrive(0, 1)
    forward(0, 1, 7)
    forward(0, 1, 6)
    make(3)
    core[0, 3].wait_recv()
    d_hop(0)
    swap_in(1)
    forward(0, 1, 3)
    forward(0, 1, 2)
    arrive(1, 1)
    forward(1, 1, 7)
    core[0, 1].wait_recv()
    n_hop(0)
    forward(1, 1, 6)
    make(5)
    core[1, 3].wait_recv()
    d_hop(1)
    forward(0, 2, 5)
    forward(0, 2, 4)
    core[0, 2].wait_recv()
    l_hop(0)
    n_hop(1)
    up = dot(fill_v[...], cot_ref[...])
    for j in range(RANKS):
        mixed = (up[j * cap : (j + 1) * cap] * slot_weight[j]).astype(bf16)
        if j == 0:
            up_v[0] = mixed
        else:
            up_s[j] = mixed
    for j in range(1, RANKS):
        up_in[j] = send(up_s.at[j], up_v.at[j], at_z[j])
    forward(1, 1, 3)
    forward(1, 1, 2)
    make(1)
    core[1, 1].wait_recv()
    l_hop(1)
    swap_in(2)
    swap_in(3)
    forward(0, 2, 1)
    forward(0, 2, 0)
    core[0, 0].wait_recv()
    g_first(0)
    g_second(0)
    arrive(2, 2)
    forward(2, 2, 7)
    forward(2, 2, 6)
    core[2, 3].wait_recv()
    d_hop(2)
    d_hop(3)
    forward(2, 2, 3)
    forward(2, 2, 2)
    g_first(1)
    core[2, 1].wait_recv()
    n_hop(2)
    forward(2, 2, 5)
    forward(2, 2, 4)
    core[2, 2].wait_recv()
    n_hop(3)
    forward(2, 2, 1)
    l_hop(2)
    l_hop(3)
    g_relay(0)
    g_second(1)
    forward(2, 2, 0)
    at_ref[...] = xs[...].T
    bt_ref[...] = bs[...].T
    g_relay(1)
    g_near(0)
    for l in (0, 1, 2, 3):
        back(0, l)
    core[2, 0].wait_recv()
    g_first(2)
    g_first(3)
    g_second(2)
    g_second(3)
    back(1, 0)
    g_near(1)
    back(0, 4)
    back(0, 5)
    g_last(0)
    back(1, 1)
    g_last(1)
    grad(0)
    back(0, 6)
    back(0, 7)
    g_make(0, g0_ref)
    g_make(1, g_s)
    g_in = send(g_s, g1_ref, at_z[1])
    g_relay(3)
    g_relay(2)
    grad(1)
    g_near(2)
    back(1, 2)
    g_near(3)
    back(1, 4)
    grad(2)
    back(1, 3)
    g_last(2)
    g_last(3)
    back(1, 5)
    for j in range(1, RANKS):
        h_in[j].wait_recv()
    out = None
    for k, w in enumerate((w0, w1)):
        column = jnp.sum(jnp.where(row_at == col_at, w, 0.0), axis=1, keepdims=True)
        picked = None
        for j in range(RANKS):
            one = dot(one_v[k, block_rows[j]], h_v[j], TN)
            picked = one if picked is None else picked + one
        picked = picked * column
        out = picked if out is None else out + picked
    hid_ref[...] = out.astype(bf16)
    back(1, 6)
    back(1, 7)
    g_make(2, g2_ref)
    g_make(3, g3_ref)
    g_in.wait_recv()
    for copy in started:
        copy.wait_send()


def run_step(ids, weight, tokens, cotangent, in_words, out_words, mean, rho, noise, cap):
    bf16, f32 = jnp.bfloat16, jnp.float32
    width, hidden = mean.shape
    count = tokens.shape[0]
    block = cotangent.shape[1]
    slots = RANKS * cap
    vmem = pl.BlockSpec(memory_space=pltpu.VMEM)
    hbm = pl.BlockSpec(memory_space=pltpu.MemorySpace.HBM)
    shape = jax.ShapeDtypeStruct
    weights = pltpu.VMEM((8, width, block), bf16)
    piece = pltpu.VMEM((8, slots, block), bf16)
    four = pltpu.VMEM((4, slots, block), bf16)
    small = pltpu.VMEM((slots, width), bf16)
    per = pltpu.VMEM((RANKS, cap, block), bf16)
    macs = slots * width * hidden
    return pl.pallas_call(
        step_kernel,
        in_specs=[vmem] * 6 + [hbm] * 3,
        out_specs=[vmem] * 12,
        out_shape=[
            pltpu.VMEM((count, block), bf16),
            pltpu.VMEM((slots, count), bf16),
            *[pltpu.VMEM((cap, width), bf16)] * RANKS,
            pltpu.VMEM((width, slots), bf16),
            pltpu.VMEM((width, slots), bf16),
            piece,
            piece,
            weights,
            weights,
        ],
        scratch_shapes=[
            weights, piece, four,
            pltpu.VMEM((RANKS, 3, cap, block), bf16),
            small, small, small, small,
            pltpu.VMEM((LANES, count), jnp.int32),
            pltpu.VMEM((2, slots, LANES), jnp.int32),
            pltpu.VMEM((slots, LANES), jnp.int32),
            per, per, per, per,
            pltpu.VMEM((2, slots, count), bf16),
            pltpu.VMEM((slots, width), f32),
            pltpu.VMEM((slots, width), f32),
            pltpu.VMEM((cap, width), bf16),
            pltpu.SemaphoreType.DMA((COPIES,)),
            pltpu.SemaphoreType.DMA((COPIES,)),
            pltpu.SemaphoreType.DMA((COPIES,)),
        ],
        compiler_params=pltpu.CompilerParams(
            collective_id=0, has_side_effects=True, vmem_limit_bytes=VMEM_LIMIT
        ),
        cost_estimate=pl.CostEstimate(
            flops=8 * macs, bytes_accessed=10 * width * hidden, transcendentals=3 * width * hidden
        ),
        name="step",
    )(ids, weight, tokens, cotangent, in_words, out_words, mean, rho, noise)


def grads_kernel(
    hid_ref, dy_ref, dyr_ref, q_ref, mean_ref, at_ref, bt_ref, hid_out, gm_out, gr_out, gm, gr, sem
):
    me = lax.axis_index("dp")
    block = dy_ref.shape[2]
    y, x, c = me // 4, (me // 2) % 2, me % 2
    copies = [pltpu.make_async_copy(hid_ref, hid_out, sem.at[16])]
    copies[0].start()

    def store(src, out, l, n):
        owner = ((y + l // 4) % 2) * 4 + ((x + (l // 2) % 2) % 2) * 2 + (c + l) % 2
        cols = pl.ds(pl.multiple_of(owner * block, LANES), block)
        copy = pltpu.make_async_copy(src, out.at[:, cols], sem.at[n])
        copy.start()
        copies.append(copy)

    for l in DONE:
        store(mean_ref.at[l], gm_out, l, 2 * l)
        store(q_ref.at[l], gr_out, l, 2 * l + 1)
    for i, l in enumerate(LEFT):
        gm[i] = dot(at_ref[...], dy_ref[l]).astype(gm.dtype)
        store(gm.at[i], gm_out, l, 2 * l)
        gd = dot(bt_ref[...], dyr_ref[l])
        gr[i] = (gd * q_ref[l].astype(jnp.float32)).astype(gr.dtype)
        store(gr.at[i], gr_out, l, 2 * l + 1)
    for copy in copies:
        copy.wait()


def grads(hid, dy, dyr, q, mean, at, bt):
    parts, slots, block = dy.shape
    width = q.shape[1]
    vmem = pl.BlockSpec(memory_space=pltpu.VMEM)
    hbm = pl.BlockSpec(memory_space=pltpu.MemorySpace.HBM)
    out = jax.ShapeDtypeStruct((width, parts * block), jnp.bfloat16)
    stage = pltpu.VMEM((len(LEFT), width, block), jnp.bfloat16)
    return pl.pallas_call(
        grads_kernel,
        in_specs=[vmem] * 7,
        out_specs=[hbm] * 3,
        out_shape=[jax.ShapeDtypeStruct(hid.shape, hid.dtype), out, out],
        scratch_shapes=[stage, stage, pltpu.SemaphoreType.DMA((17,))],
        compiler_params=pltpu.CompilerParams(vmem_limit_bytes=20 * 1024 * 1024),
        cost_estimate=pl.CostEstimate(
            flops=4 * slots * width * parts * block,
            bytes_accessed=6 * width * parts * block,
            transcendentals=0,
        ),
        name="grads",
    )(hid, dy, dyr, q, mean, at, bt)


def on_device(
    tokens,
    in_signs,
    out_signs,
    expert_ids,
    route_weight,
    cotangent,
    mean_weight,
    rho_weight,
    noise_weight,
):
    parts = lax.axis_size("dp")
    ranks = lax.axis_size("expert")
    count, width = tokens.shape
    topk = expert_ids.shape[1]
    hidden = mean_weight.shape[2]
    block = cotangent.shape[1]
    capacity = 5 * count * topk // (4 * ranks)
    half = out_signs.shape[1] // 2
    fits = parts == 8 and ranks == RANKS and mean_weight.shape[0] == 1 and topk == 2
    fits = fits and block % LANES == 0 and width % LANES == 0 and count == LANES
    fits = fits and half + in_signs.shape[1] == LANES and half % 8 == 0 and capacity % 16 == 0
    if not fits or hidden % 512:
        return on_device_general(
            tokens,
            in_signs,
            out_signs,
            expert_ids,
            route_weight,
            cotangent,
            mean_weight,
            rho_weight,
            noise_weight,
        )
    hidden_out, fill, g0, g1, g2, g3, at, bt, dy, dyr, q, mean = run_step(
        expert_ids.T,
        route_weight.T,
        tokens,
        cotangent,
        in_signs.T,
        out_signs.T,
        mean_weight[0],
        rho_weight[0],
        noise_weight[0],
        capacity,
    )
    pieces = [g0, g1]
    for j, piece in ((2, g2), (3, g3)):
        pieces.append(lax.ppermute(piece, "expert", [(z, z ^ j) for z in range(ranks)]))
    hidden_out, grad_mean, grad_rho = grads(hidden_out, dy, dyr, q, mean, at, bt)
    grad_tokens = dot(fill, jnp.concatenate(pieces, axis=0), TN).astype(jnp.bfloat16)
    return (hidden_out, grad_tokens, grad_mean[None], grad_rho[None])


def solution(mesh):
    in_specs = (
        P("expert", "dp"),
        P("expert", "dp"),
        P("expert", None),
        P("expert", None),
        P("expert", None),
        P("expert", "dp"),
        P("expert", "dp", None),
        P("expert", "dp", None),
        P("expert", "dp", None),
    )
    out_specs = (
        P("expert", "dp"),
        P("expert", "dp"),
        P("expert", "dp", None),
        P("expert", "dp", None),
    )
    return jax.shard_map(
        on_device, mesh=mesh, in_specs=in_specs, out_specs=out_specs, check_vma=False
    )
```
